256 devices in a mesh: replica: 16 (over x_hi, z), tensor: 16 (over y, x_lo, core).
Axes of the slice: x: 4 (x_hi: 2, x_lo: 2; x = x_hi * 2 + x_lo), y: 4, z: 8, core: 2. Of those that a mesh axis runs over, the one named last changes fastest.
Arguments:
- hidden: bfloat16 [512, 8192], P('replica'), may hold values from -16 to 16
- q_weight: bfloat16 [8192, 4096], P(None, 'tensor'), may hold values from -0.0625 to 0.0625
- q_gain: float32 [128], replicated, may hold values from 0.1 to 1.9
- o_weight: bfloat16 [4096, 8192], P('tensor'), may hold values from -0.125 to 0.125
- attn_gate: float32 [1], replicated, may hold values from 0.5 to 1.5
- key_codes: bfloat16 [128, 512, 1024], P('replica', 'tensor'), may hold values from -96 to 96
- value_codes: bfloat16 [128, 512, 1024], P('replica', 'tensor'), may hold values from -96 to 96
- key_scales: bfloat16 [128, 16, 8], P('replica', 'tensor'), may hold values from 0.02 to 8
- value_scales: bfloat16 [128, 16, 8], P('replica', 'tensor'), may hold values from 0.019897461 to 0.119628906
- lengths: int32 [128], P('replica'), may hold values from 128 to 512
- dest_replica: int32 [16, 6], replicated, may hold values from 0 to 15, as said below
- move_slot: int32 [16, 6], P('replica'), may hold values from 0 to 7, as said below
Outputs:
- mixed: bfloat16 [512, 8192], P('replica', 'tensor')
- new_keys: bfloat16 [128, 512, 1024], P('replica', 'tensor')
- new_values: bfloat16 [128, 512, 1024], P('replica', 'tensor')
- new_key_scales: bfloat16 [128, 16, 8], P('replica', 'tensor')
- new_value_scales: bfloat16 [128, 16, 8], P('replica', 'tensor')
The draws below stay inside these ranges and needn't reach their ends.
Inputs may be any that keep to these rules, and one draw needn't show every extreme that they name: For each j the column dest_replica[:, j] names every replica once, so each replica receives exactly 6 requests, at most one from each replica; a request may stay on its own replica. `move_slot`: the 6 slots of one replica are different.
All inputs are finite; a program needn't handle non-finite values.
Results may differ from the reference program's by a relative error of at most 0.0065.
Values may be sent and summed in bfloat16 or wider, within the bound.
No kernel may reach another device: no remote copies, remote signals or barrier semaphores. Data moves between devices by JAX's collectives and lax.ppermute only.
A program may use at most 64 MiB of HBM per device.

```python
import math
import jax
import jax.numpy as jnp
from jax import lax

D = 8192
HQ = 32
KVH = 8
HD = 128
IMG_DEV = 32
REQ_REP = 8
SPEC = 4
MOVE = 6
REPLICAS = 16
REQUESTS = 128
IMG = 512
TSHARDS = 16
ROWS = 512


def draw_hidden(key, part):
    first, second = jax.random.split(jax.random.fold_in(key, 11), 2)
    scales = jnp.exp(jax.random.uniform(first, (ROWS, 1), jnp.float32, math.log(0.25), math.log(4.0)))
    values = jnp.clip(jax.random.normal(second, (ROWS, D), jnp.float32), -4.0, 4.0) * scales
    return values.astype(jnp.bfloat16)


def draw_key_scales(key, part):
    first = jax.random.fold_in(jax.random.fold_in(key, 23), 0)
    base = jnp.exp(jax.random.uniform(first, (REQUESTS, TSHARDS, KVH), jnp.float32, math.log(0.02), math.log(0.12)))
    return base.astype(jnp.bfloat16)


def draw_dest_replica(key, part):
    first, second, third = jax.random.split(jax.random.fold_in(key, 37), 3)
    relabel = jax.random.permutation(first, REPLICAS)
    order = jax.random.permutation(second, REPLICAS)
    offsets = jax.random.permutation(third, REPLICAS)[:MOVE]
    return relabel[(order[:, None] + offsets[None, :]) % REPLICAS].astype(jnp.int32)


def draw_move_slot(key, part):
    keys = jax.random.split(jax.random.fold_in(key, 41), REPLICAS)
    return jax.vmap(lambda item: jax.random.permutation(item, REQ_REP)[:MOVE])(keys).astype(jnp.int32)


def place_ends(entries, own_key, low, largest):
    index_at = [jax.random.randint(jax.random.fold_in(own_key, axis), (), 0, length) for axis, length in enumerate(entries.shape)]
    longest = entries.shape.index(max(entries.shape))
    beside = index_at[:longest] + [(index_at[longest] + 1) % entries.shape[longest]] + index_at[longest + 1:]
    return entries.at[tuple(index_at)].set(low).at[tuple(beside)].set(largest)


def strengthened(array, rng, source, target, parts, factor):
    def block_of(axis_at):
        return (jnp.arange(array.shape[axis_at]) // (array.shape[axis_at] // parts)).reshape((-1,) + (1,) * (array.ndim - 1 - axis_at))

    near = jax.random.permutation(rng, parts)[block_of(target)]
    far = (block_of(target) + parts // 2) % parts
    return jnp.where((block_of(source) == near) | (block_of(source) == far), factor * array, array)


def block_scale(own_key, shape, shards, least, largest):
    def one(axis_at, blocks):
        steps = jax.random.uniform(jax.random.fold_in(jax.random.fold_in(own_key, 6), axis_at), (blocks,), jnp.float32, least / len(shards), largest / len(shards))
        return jnp.repeat(jnp.exp(steps), shape[axis_at] // blocks).reshape((-1,) + (1,) * (len(shape) - axis_at - 1))

    gain = one(*shards[0])
    for cut in shards[1:]:
        gain = gain * one(*cut)
    return gain


def centred(key, dims, spread, limit, cuts=(), kind=jnp.bfloat16):
    loudness = block_scale(key, dims, cuts, -0.22, 0.18) if cuts else 1.0
    array = jax.random.normal(key, dims, jnp.float32) * spread * loudness
    return jnp.minimum(jnp.maximum(array, -limit), limit).astype(kind)


def gaussian_with(rng, shape, scale, most, shards, heavy, kind=jnp.bfloat16):
    array = scale * jax.random.normal(rng, shape, jnp.float32)
    if shards:
        array = array * block_scale(rng, shape, shards, -0.22, 0.18)
    return jnp.clip(strengthened(array, jax.random.fold_in(rng, 3), *heavy), -most, most).astype(kind)


def setup_inputs(seed: int = 0) -> dict:
    seeds = jax.random.split(jax.random.key(seed), 13)
    hidden = draw_hidden(jax.random.fold_in(seeds[12], 71), 0)
    q_weight = centred(seeds[1], (D, HQ * HD), D ** -0.5, 0.0625, ((1, 16),))
    q_gain = jnp.clip(1.0 + 0.18 * jax.random.normal(seeds[2], (HD,), jnp.float32), 0.1, 1.9)
    o_weight = gaussian_with(seeds[3], (HQ * HD, D), (HQ * HD) ** -0.5, 0.125, ((0, 16),), (0, 1, 16, 2.0))
    attn_gate = jnp.clip(jax.random.uniform(seeds[4], (1,), jnp.float32, 0.5, 1.5), 0.5, 1.5)
    key_codes = centred(seeds[5], (REQUESTS, IMG, KVH * HD), 16.0, 96.0, ((0, 16), (1, 16)))
    value_codes = centred(seeds[6], (REQUESTS, IMG, KVH * HD), 16.0, 96.0, ((0, 16), (1, 16)))
    key_scales = draw_key_scales(jax.random.fold_in(seeds[12], 71), 0)
    value_scales = jnp.clip(jnp.exp(math.log(0.119628906) - 1.7938024 * jax.random.uniform(seeds[8], (REQUESTS, TSHARDS, KVH), jnp.float32) ** block_scale(seeds[8], (REQUESTS, TSHARDS, KVH), ((0, 16), (1, 16)), -0.2, 0.2)), 0.019897461, 0.119628906).astype(jnp.bfloat16)
    lengths = place_ends(jax.random.randint(seeds[9], (REQUESTS,), IMG // 4, IMG + 1), jax.random.fold_in(seeds[9], 1), IMG // 4, IMG).astype(jnp.int32)
    dest_replica = draw_dest_replica(jax.random.fold_in(seeds[12], 71), 0)
    move_slot = draw_move_slot(jax.random.fold_in(seeds[12], 71), 0)
    return dict(hidden=hidden, q_weight=q_weight, q_gain=q_gain, o_weight=o_weight, attn_gate=attn_gate, key_codes=key_codes, value_codes=value_codes, key_scales=key_scales, value_scales=value_scales, lengths=lengths, dest_replica=dest_replica, move_slot=move_slot)


NEGATIVE = -1e+30
EPSILON = 1e-06

def one_request(item):
    query, keys, values, key_scale, value_scale, length = item
    keys = keys.reshape(TSHARDS, IMG_DEV, KVH, HD).astype(jnp.float32)
    values = values.reshape(TSHARDS, IMG_DEV, KVH, HD).astype(jnp.float32)
    scores = jnp.einsum('sngd,btnd->sngbt', query.astype(jnp.float32), keys, precision=lax.Precision.HIGHEST)
    scores = scores * key_scale.astype(jnp.float32).T[None, :, None, :, None]
    position = jnp.arange(IMG, dtype=jnp.int32).reshape(TSHARDS, IMG_DEV)
    valid = position < length
    block_max = lax.optimization_barrier(jnp.max(jnp.where(valid, scores, NEGATIVE), axis=-1))
    weights = jnp.where(valid, jnp.exp(scores - block_max[..., None]), 0.0)
    block_sum = lax.optimization_barrier(jnp.sum(weights, axis=-1))
    rounded = weights.astype(jnp.bfloat16).astype(jnp.float32)
    block_out = jnp.einsum('sngbt,btnd->sngbd', rounded, values, precision=lax.Precision.HIGHEST)
    block_out = block_out * value_scale.astype(jnp.float32).T[None, :, None, :, None]
    top = lax.optimization_barrier(jnp.max(block_max, axis=-1))
    factor = jnp.exp(block_max - top[..., None])
    total = lax.optimization_barrier(jnp.sum(block_sum * factor, axis=-1))
    summed = lax.optimization_barrier(jnp.sum(block_out * factor[..., None], axis=3))
    return (summed / total[..., None]).astype(jnp.bfloat16)

def reference(hidden, q_weight, q_gain, o_weight, attn_gate, key_codes, value_codes, key_scales, value_scales, lengths, dest_replica, move_slot):
    projected = jnp.dot(hidden, q_weight, preferred_element_type=jnp.float32).reshape(ROWS, HQ, HD)
    projected = projected * lax.rsqrt(lax.optimization_barrier(jnp.mean(projected * projected, axis=-1, keepdims=True)) + EPSILON)
    query = (projected * q_gain.astype(jnp.float32) * HD ** (-0.5)).astype(jnp.bfloat16)
    grouped = query.reshape(REQUESTS, SPEC, KVH, HQ // KVH, HD)
    attended = lax.map(one_request, (grouped, key_codes, value_codes, key_scales, value_scales, lengths))
    attended = attended.reshape(ROWS, HQ * HD)
    summed = jnp.dot(attended, o_weight, preferred_element_type=jnp.float32)
    mixed = (hidden.astype(jnp.float32) + jnp.tanh(attn_gate[0]) * summed).astype(jnp.bfloat16)
    columns = jnp.arange(MOVE, dtype=jnp.int32)[None, :]
    source_rows = (jnp.arange(REPLICAS, dtype=jnp.int32)[:, None] * REQ_REP + move_slot).reshape(-1)
    target_rows = (dest_replica * REQ_REP + move_slot[dest_replica, columns]).reshape(-1)
    order = jnp.arange(REQUESTS, dtype=jnp.int32).at[target_rows].set(source_rows)
    return (mixed, key_codes[order], value_codes[order], key_scales[order], value_scales[order])
```

```python
import functools

import jax
import jax.numpy as jnp
from jax import lax
from jax.experimental import pallas as pl
from jax.experimental.pallas import tpu as pltpu
from jax.sharding import PartitionSpec as P

NEGATIVE = -1e30
EPSILON = 1e-06
BF16, F32, I32 = jnp.bfloat16, jnp.float32, jnp.int32

REPLICAS = 16
MOVE = 6
HELD = 8
SPAN = 32
SPEC = 4
ROWS = HELD * SPEC
KVH = 8
HD = 128
TENSORS = 16
SLOT = 2 * KVH * SPAN + 8
COLS = 512


VMEM = pl.BlockSpec(memory_space=pltpu.VMEM)
SMEM = pl.BlockSpec(memory_space=pltpu.SMEM)
ANY = pl.BlockSpec(memory_space=pl.ANY)


def cost(flops, moved):
    return pl.CostEstimate(flops=flops, bytes_accessed=moved, transcendentals=0)


def room(mib):
    return pltpu.CompilerParams(vmem_limit_bytes=mib << 20)


def shape(dims, dtype):
    return jax.ShapeDtypeStruct(dims, dtype)


def iota(dims, axis):
    return lax.broadcasted_iota(I32, dims, axis)


def scale_rows(scr, key_scales, value_scales):
    scr[...] = jnp.zeros_like(scr)
    scr[0:HELD, 0:KVH] = key_scales[...].astype(F32)
    scr[HELD : 2 * HELD, 0:KVH] = value_scales[...].astype(F32)


def pack_kernel(
    at, dest, slots, keys, values, key_scales, value_scales, out, held, stage, scr, in_sem, out_sem
):
    here = at[0]
    loads = []
    for j in range(MOVE):
        s = slots[0, j]
        pair = (
            pltpu.make_async_copy(keys.at[s], held.at[j, 0], in_sem.at[j, 0]),
            pltpu.make_async_copy(values.at[s], held.at[j, 1], in_sem.at[j, 1]),
        )
        for copy in pair:
            copy.start()
        loads.append(pair)
    scale_rows(scr, key_scales, value_scales)
    row = iota((8, HD), 0)
    stores = []
    for j in range(MOVE):
        s = slots[0, j]
        both = jnp.where(
            row == 0,
            scr[pl.ds(s, 1), :],
            jnp.where(row == 1, scr[pl.ds(HELD + s, 1), :], 0.0),
        )
        stage[j, 2 * KVH * SPAN : SLOT, :] = both.astype(BF16)
        for which in range(2):
            loads[j][which].wait()
            for c in range(KVH):
                at_row = (which * KVH + c) * SPAN
                stage[j, at_row : at_row + SPAN, :] = held[j, which, :, c * HD : (c + 1) * HD]
        copy = pltpu.make_async_copy(stage.at[j], out.at[dest[j, here]], out_sem.at[j])
        copy.start()
        stores.append(copy)
    for copy in stores:
        copy.wait()


def pack(at, dest, slots, keys, values, key_scales, value_scales):
    return pl.pallas_call(
        pack_kernel,
        out_shape=shape((REPLICAS, SLOT, HD), BF16),
        in_specs=[SMEM, SMEM, SMEM, ANY, ANY, VMEM, VMEM],
        out_specs=ANY,
        scratch_shapes=[
            pltpu.VMEM((MOVE, 2, SPAN, KVH * HD), BF16),
            pltpu.VMEM((MOVE, SLOT, HD), BF16),
            pltpu.VMEM((2 * HELD, HD), F32),
            pltpu.SemaphoreType.DMA((MOVE, 2)),
            pltpu.SemaphoreType.DMA((MOVE,)),
        ],
        cost_estimate=cost(1 << 20, 4 << 20),
        name="pack",
    )(at, dest, slots, keys, values, key_scales, value_scales)


def unpack_kernel(
    at,
    dest,
    slots,
    received,
    keys,
    values,
    key_scales,
    value_scales,
    new_keys,
    new_values,
    new_key_scales,
    new_value_scales,
    landed,
    stage,
    kept,
    scr,
    in_sem,
    out_sem,
    kept_sem,
):
    here = at[0]
    loads = []
    for j in range(MOVE):
        source = jnp.int32(0)
        for p in range(REPLICAS):
            source = jnp.where(dest[j, p] == here, p, source)
        copy = pltpu.make_async_copy(received.at[source], landed.at[j], in_sem.at[j])
        copy.start()
        loads.append(copy)
    stays = []
    for r in range(HELD):
        moving = slots[0, 0] == r
        for j in range(1, MOVE):
            moving = jnp.logical_or(moving, slots[0, j] == r)
        stays.append(jnp.logical_not(moving))

    def kept_in(r):
        return (
            pltpu.make_async_copy(keys.at[r], kept.at[r, 0], kept_sem.at[r, 0]),
            pltpu.make_async_copy(values.at[r], kept.at[r, 1], kept_sem.at[r, 1]),
        )

    def kept_out(r):
        return (
            pltpu.make_async_copy(kept.at[r, 0], new_keys.at[r], kept_sem.at[r, 0]),
            pltpu.make_async_copy(kept.at[r, 1], new_values.at[r], kept_sem.at[r, 1]),
        )

    for r in range(HELD):

        @pl.when(stays[r])
        def _():
            for copy in kept_in(r):
                copy.start()

    scale_rows(scr, key_scales, value_scales)
    for r in range(HELD):

        @pl.when(stays[r])
        def _():
            for copy in kept_in(r):
                copy.wait()
            for copy in kept_out(r):
                copy.start()

    stores = []
    for j in range(MOVE):
        s = slots[0, j]
        loads[j].wait()
        both = landed[j, 2 * KVH * SPAN : SLOT, :].astype(F32)
        scr[pl.ds(s, 1), :] = both[0:1, :]
        scr[pl.ds(HELD + s, 1), :] = both[1:2, :]
        for which, target in ((0, new_keys), (1, new_values)):
            for c in range(KVH):
                at_row = (which * KVH + c) * SPAN
                stage[j, which, :, c * HD : (c + 1) * HD] = landed[j, at_row : at_row + SPAN, :]
            copy = pltpu.make_async_copy(stage.at[j, which], target.at[s], out_sem.at[j, which])
            copy.start()
            stores.append(copy)
    new_key_scales[...] = scr[0:HELD, 0:KVH].astype(BF16)
    new_value_scales[...] = scr[HELD : 2 * HELD, 0:KVH].astype(BF16)
    for r in range(HELD):

        @pl.when(stays[r])
        def _():
            for copy in kept_out(r):
                copy.wait()

    for copy in stores:
        copy.wait()


def unpack(at, dest, slots, received, keys, values, key_scales, value_scales):
    return pl.pallas_call(
        unpack_kernel,
        out_shape=(
            shape(keys.shape, BF16),
            shape(values.shape, BF16),
            shape((HELD, KVH), BF16),
            shape((HELD, KVH), BF16),
        ),
        in_specs=[SMEM, SMEM, SMEM, ANY, ANY, ANY, VMEM, VMEM],
        out_specs=(ANY, ANY, VMEM, VMEM),
        scratch_shapes=[
            pltpu.VMEM((MOVE, SLOT, HD), BF16),
            pltpu.VMEM((MOVE, 2, SPAN, KVH * HD), BF16),
            pltpu.VMEM((HELD, 2, SPAN, KVH * HD), BF16),
            pltpu.VMEM((2 * HELD, HD), F32),
            pltpu.SemaphoreType.DMA((MOVE,)),
            pltpu.SemaphoreType.DMA((MOVE, 2)),
            pltpu.SemaphoreType.DMA((HELD, 2)),
        ],
        cost_estimate=cost(1 << 20, 4 << 20),
        compiler_params=room(8),
        name="unpack",
    )(at, dest, slots, received, keys, values, key_scales, value_scales)


def query_kernel(hidden, weight, gain, query, total):
    step = pl.program_id(0)

    @pl.when(step == 0)
    def _():
        total[...] = jnp.zeros_like(total)

    total[...] += jnp.dot(hidden[...], weight[...], preferred_element_type=F32)

    @pl.when(step == pl.num_programs(0) - 1)
    def _():
        for h in range(2):
            part = total[:, h * HD : (h + 1) * HD]
            mean = jnp.mean(part * part, axis=-1, keepdims=True)
            part = part * lax.rsqrt(mean + EPSILON)
            query[:, h * HD : (h + 1) * HD] = (part * gain[...] * HD ** (-0.5)).astype(BF16)


def project_query(hidden, q_weight, q_gain):
    depth = hidden.shape[1]
    steps = 8
    block = depth // steps
    return pl.pallas_call(
        query_kernel,
        grid=(steps,),
        out_shape=shape((ROWS, 2 * HD), BF16),
        in_specs=[
            pl.BlockSpec((ROWS, block), lambda i: (0, i)),
            pl.BlockSpec((block, 2 * HD), lambda i: (i, 0)),
            pl.BlockSpec((1, HD), lambda i: (0, 0)),
        ],
        out_specs=pl.BlockSpec((ROWS, 2 * HD), lambda i: (0, 0)),
        scratch_shapes=[pltpu.VMEM((ROWS, 2 * HD), F32)],
        cost_estimate=cost(4 << 20, 4 << 20),
        compiler_params=room(8),
        name="query",
    )(hidden, q_weight, q_gain.reshape(1, HD))


def split3(x):
    high = x.astype(BF16).astype(F32)
    rest = x - high
    middle = rest.astype(BF16).astype(F32)
    return high, middle, rest - middle


def put_stats(out, at_row, stats):
    high, middle, low = split3(stats)
    out[at_row : at_row + 16, :] = jnp.concatenate([high, middle], axis=0).astype(BF16)
    out[at_row + 16 : at_row + 32, :] = jnp.concatenate(
        [low, jnp.zeros_like(low)], axis=0
    ).astype(BF16)


def get_stats(message, at_row):
    first = message[at_row : at_row + 16, :].astype(F32)
    second = message[at_row + 16 : at_row + 32, :].astype(F32)
    return (first[0:8] + first[8:16]) + second[0:8]


def columns_of(rows):
    short = HD - rows.shape[0]
    return jnp.concatenate([rows, jnp.zeros((short, HD), F32)], axis=0).T


def attend_kernel(
    at, lengths, q0, q1, q2, q3, keys, values, key_scales, value_scales,
    o0, o1, o2, o3, q_all, o_all, mask, stats,
):
    rank = at[1]
    y = rank // 4
    x = (rank // 2) % 2
    for k, q in enumerate((q0, q1, q2, q3)):
        q_all[k] = q[...]
    tokens = HELD * SPAN
    row_request = (iota((HD, tokens), 0) // SPEC) % HELD
    col = iota((HD, tokens), 1)
    limit = jnp.zeros((1, tokens), I32)
    col1 = iota((1, tokens), 1)
    for r in range(HELD):
        limit = jnp.where(col1 // SPAN == r, lengths[r], limit)
    in_reach = rank * SPAN + col1 % SPAN < limit
    ok = jnp.logical_and(row_request == col // SPAN, in_reach)
    mask[...] = jnp.where(ok, 1.0, 0.0)
    spread_cols = (iota((HELD, tokens), 1) // SPAN == iota((HELD, tokens), 0)).astype(BF16)
    spread_rows = ((iota((HD, HELD), 0) // SPEC) % HELD == iota((HD, HELD), 1)).astype(BF16)
    col_scale = lax.dot_general(
        key_scales[...], spread_cols, (((0,), (0,)), ((), ())), preferred_element_type=F32
    )
    row_scale = jnp.dot(spread_rows, value_scales[...], preferred_element_type=F32)
    lane = iota((HD, HD), 1)
    stats[...] = jnp.zeros_like(stats)
    for m in range(KVH):
        k = (y - m // 2 + 4) % 4
        dx = (m % 2 + x) % 2
        near = q_all[k, 2 * dx]
        far = q_all[k, 2 * dx + 1]
        grouped = jnp.concatenate(
            [near[:, :HD], near[:, HD:], far[:, :HD], far[:, HD:]], axis=0
        )
        key = keys[:, :, m * HD : (m + 1) * HD].reshape(tokens, HD)
        value = values[:, :, m * HD : (m + 1) * HD].reshape(tokens, HD)
        scores = lax.dot_general(
            grouped, key, (((1,), (1,)), ((), ())), preferred_element_type=F32
        )
        scores = scores * col_scale[m : m + 1, :]
        good = mask[...] > 0.5
        peak = jnp.max(jnp.where(good, scores, NEGATIVE), axis=1, keepdims=True)
        weight = jnp.where(good, jnp.exp(scores - peak), 0.0)
        total = jnp.sum(weight, axis=1, keepdims=True)
        out = jnp.dot(weight.astype(BF16), value, preferred_element_type=F32)
        o_all[k, dx] = (out * row_scale[:, m : m + 1]).astype(BF16)
        first = 8 * k + 2 * dx
        stats[...] = jnp.where(
            lane == first, peak, jnp.where(lane == first + 1, total, stats[...])
        )
    turned = stats[...].T
    for k, o in enumerate((o0, o1, o2, o3)):
        o[0:HD, :] = o_all[k, 0]
        o[HD : 2 * HD, :] = o_all[k, 1]
        put_stats(o, 2 * HD, turned[8 * k : 8 * k + 8])


def attend(at, lengths, queries, keys, values, key_scales, value_scales):
    out = shape((2 * HD + 32, HD), BF16)
    return pl.pallas_call(
        attend_kernel,
        out_shape=(out,) * 4,
        in_specs=[SMEM, SMEM] + [VMEM] * 8,
        out_specs=(VMEM,) * 4,
        scratch_shapes=[
            pltpu.VMEM((4, 4, ROWS, 2 * HD), BF16),
            pltpu.VMEM((4, 2, HD, HD), BF16),
            pltpu.VMEM((HD, HELD * SPAN), F32),
            pltpu.VMEM((HD, HD), F32),
        ],
        cost_estimate=cost(4 << 20, 2 << 20),
        compiler_params=room(8),
        name="attend",
    )(at, lengths, *queries, keys, values, key_scales, value_scales)


def merged(stats):
    top = functools.reduce(jnp.maximum, stats)
    factors = [jnp.exp(s - top) for s in stats]
    total = sum(s * pltpu.roll(f, 1, 0) for s, f in zip(stats, factors))
    peak_row = iota(top.shape, 0) % 2 == 0
    return factors, jnp.where(peak_row, top, total)


def combine_kernel(p0, p1, p2, p3, o0, o1, o2, o3):
    parts = (p0, p1, p2, p3)
    factors, both = merged([get_stats(p, 2 * HD) for p in parts])
    column = columns_of(jnp.concatenate(factors, axis=0))
    outs = ((o0, o1), (o2, o3))
    for dx in range(2):
        summed = jnp.zeros((HD, HD), F32)
        for k, p in enumerate(parts):
            part = p[dx * HD : (dx + 1) * HD, :].astype(F32)
            summed = summed + part * column[:, 8 * k + 2 * dx : 8 * k + 2 * dx + 1]
        for dc in range(2):
            outs[dx][dc][0 : HD // 2, :] = summed[dc * 64 : dc * 64 + 64].astype(BF16)
            put_stats(outs[dx][dc], HD // 2, both)


def combine(parts):
    out = shape((HD // 2 + 32, HD), BF16)
    return pl.pallas_call(
        combine_kernel,
        out_shape=(out,) * 4,
        in_specs=[VMEM] * 4,
        out_specs=(VMEM,) * 4,
        cost_estimate=cost(1 << 20, 1 << 19),
        compiler_params=room(4),
        name="combine",
    )(*parts)


def finish_kernel(p0, p1, p2, p3, attended):
    parts = (p0, p1, p2, p3)
    stats = []
    for d, p in enumerate(parts):
        s = get_stats(p, HD // 2)
        if d // 2:
            s = pltpu.roll(s, 6, 0)
        if d % 2:
            s = pltpu.roll(s, HD // 2, 1)
        stats.append(s)
    factors, both = merged(stats)
    over = pltpu.roll(both, 7, 0)
    column = columns_of(jnp.concatenate([f / over for f in factors], axis=0))
    summed = jnp.zeros((HD // 2, HD), F32)
    for d, p in enumerate(parts):
        summed = summed + p[0 : HD // 2, :].astype(F32) * column[0 : HD // 2, 8 * d : 8 * d + 1]
    for h in range(2):
        attended[:, h * HD : (h + 1) * HD] = summed[h * ROWS : (h + 1) * ROWS].astype(BF16)


def finish(parts):
    return pl.pallas_call(
        finish_kernel,
        out_shape=shape((ROWS, 2 * HD), BF16),
        in_specs=[VMEM] * 4,
        out_specs=VMEM,
        cost_estimate=cost(1 << 20, 1 << 19),
        compiler_params=room(4),
        name="finish",
    )(*parts)


def output_kernel(other, at, attended, weight, out, blocks, sem):
    core = (at[1] + other) % 2
    copies = []
    for i in range(TENSORS // 2):
        start = pl.multiple_of((2 * i + core) * COLS, COLS)
        copy = pltpu.make_async_copy(weight.at[:, pl.ds(start, COLS)], blocks.at[i], sem.at[i])
        copy.start()
        copies.append(copy)
    for i in range(TENSORS // 2):
        copies[i].wait()
        out[i] = jnp.dot(attended[...], blocks[i], preferred_element_type=F32).astype(out.dtype)


def project_output(other, dtype, at, attended, o_weight):
    half = TENSORS // 2
    return pl.pallas_call(
        functools.partial(output_kernel, other),
        out_shape=shape((half, ROWS, COLS), dtype),
        in_specs=[SMEM, VMEM, ANY],
        out_specs=VMEM,
        scratch_shapes=[
            pltpu.VMEM((half, 2 * HD, COLS), BF16),
            pltpu.SemaphoreType.DMA((half,)),
        ],
        cost_estimate=cost(1 << 22, 2 << 20),
        compiler_params=room(8),
        name="output_other" if other else "output_own",
    )(at, attended, o_weight)


def share_kernel(at, own, received, keep, s1, s2, s3):
    y = at[1] // 4
    for k in range(4):
        group = (y - k + 4) % 4
        for c in range(2):
            value = own[2 * group + c] + received[2 * group + c].astype(F32)
            if k == 0:
                keep[c] = value
            else:
                (s1, s2, s3)[k - 1][c] = value.astype(BF16)


def share(at, own, received):
    out = shape((2, ROWS, COLS), BF16)
    return pl.pallas_call(
        share_kernel,
        out_shape=(shape((2, ROWS, COLS), F32), out, out, out),
        in_specs=[SMEM, VMEM, VMEM],
        out_specs=(VMEM,) * 4,
        cost_estimate=cost(1 << 20, 1 << 20),
        compiler_params=room(6),
        name="share",
    )(at, own, received)


def narrow_kernel(at, own, r1, r2, r3, keep, send):
    x = (at[1] // 2) % 2
    for c, out in ((x, keep), (1 - x, send)):
        value = own[c] + r1[c].astype(F32) + r2[c].astype(F32) + r3[c].astype(F32)
        out[...] = value.astype(out.dtype)


def narrow(at, own, received):
    return pl.pallas_call(
        narrow_kernel,
        out_shape=(shape((ROWS, COLS), F32), shape((ROWS, COLS), BF16)),
        in_specs=[SMEM] + [VMEM] * 4,
        out_specs=(VMEM,) * 2,
        cost_estimate=cost(1 << 20, 1 << 19),
        compiler_params=room(4),
        name="narrow",
    )(at, own, *received)


def mix_kernel(at, gate, own, received, hidden, out, rows, sem):
    start = pl.multiple_of(at[1] * COLS, COLS)
    copy = pltpu.make_async_copy(hidden.at[:, pl.ds(start, COLS)], rows, sem)
    copy.start()
    scale = jnp.tanh(jnp.full((8, HD), gate[0], F32))[0:1, 0:1]
    summed = own[...] + received[...].astype(F32)
    copy.wait()
    out[...] = (rows[...].astype(F32) + scale * summed).astype(BF16)


def mix(at, gate, own, received, hidden):
    return pl.pallas_call(
        mix_kernel,
        out_shape=shape((ROWS, COLS), BF16),
        in_specs=[SMEM, SMEM, VMEM, VMEM, ANY],
        out_specs=VMEM,
        scratch_shapes=[pltpu.VMEM((ROWS, COLS), BF16), pltpu.SemaphoreType.DMA],
        cost_estimate=cost(1 << 20, 1 << 18),
        compiler_params=room(4),
        name="mix",
    )(at, gate, own, received, hidden)


def swap(array, bits):
    return lax.ppermute(array, "tensor", [(i, i ^ bits) for i in range(TENSORS)])


def shift(array, rows):
    return lax.ppermute(array, "tensor", [(i, (i + 4 * rows) % TENSORS) for i in range(TENSORS)])


def attention(
    at, hidden, q_weight, q_gain, o_weight, attn_gate, keys, values, key_scales, value_scales, lengths
):
    query = project_query(hidden, q_weight, q_gain)
    local = jnp.stack([query] + [swap(query, d) for d in (1, 2, 3)])
    queries = [local] + [shift(local, k) for k in (1, 2, 3)]
    parts = attend(at, lengths, queries, keys, values, key_scales, value_scales)
    parts = combine([parts[0]] + [shift(parts[k], -k) for k in (1, 2, 3)])
    attended = finish([parts[0]] + [swap(parts[d], d) for d in (1, 2, 3)])
    other = swap(project_output(1, BF16, at, attended, o_weight), 1)
    own = project_output(0, F32, at, attended, o_weight)
    own, *sent = share(at, own, other)
    own, sent = narrow(at, own, [shift(s, -k) for k, s in zip((1, 2, 3), sent)])
    return mix(at, attn_gate, own, swap(sent, 2), hidden)


def local(
    hidden,
    q_weight,
    q_gain,
    o_weight,
    attn_gate,
    key_codes,
    value_codes,
    key_scales,
    value_scales,
    lengths,
    dest_replica,
    move_slot,
):
    at = jnp.stack([lax.axis_index("replica"), lax.axis_index("tensor")]).astype(I32)
    dest = dest_replica.T
    key_scales, value_scales = key_scales[:, 0, :], value_scales[:, 0, :]
    message = pack(at, dest, move_slot, key_codes, value_codes, key_scales, value_scales)
    received = lax.all_to_all(
        message, "replica", split_axis=0, concat_axis=0, tiled=True
    )
    mixed = attention(
        at, hidden, q_weight, q_gain, o_weight, attn_gate,
        key_codes, value_codes, key_scales, value_scales, lengths,
    )
    new_keys, new_values, new_ks, new_vs = unpack(
        at, dest, move_slot, received, key_codes, value_codes, key_scales, value_scales
    )
    return (mixed, new_keys, new_values, new_ks[:, None, :], new_vs[:, None, :])


def solution(mesh):
    return jax.shard_map(
        local,
        mesh=mesh,
        in_specs=(
            P("replica", None),
            P(None, "tensor"),
            P(),
            P("tensor", None),
            P(),
            P("replica", "tensor", None),
            P("replica", "tensor", None),
            P("replica", "tensor", None),
            P("replica", "tensor", None),
            P("replica"),
            P(),
            P("replica", None),
        ),
        out_specs=(
            P("replica", "tensor"),
            P("replica", "tensor", None),
            P("replica", "tensor", None),
            P("replica", "tensor", None),
            P("replica", "tensor", None),
        ),
        check_vma=False,
    )
```

```python
import functools

import jax
import jax.numpy as jnp
from jax import lax
from jax.experimental import pallas as pl
from jax.experimental.pallas import tpu as pltpu
from jax.sharding import PartitionSpec as P

NEGATIVE = -1e30
EPSILON = 1e-06
BF16, F32, I32 = jnp.bfloat16, jnp.float32, jnp.int32

REPLICAS = 16
MOVE = 6
HELD = 8
SPAN = 32
SPEC = 4
ROWS = HELD * SPEC
KVH = 8
HD = 128
TENSORS = 16
SLOT = 2 * KVH * SPAN + 8
COLS = 512
STEPS = 8


VMEM = pl.BlockSpec(memory_space=pltpu.VMEM)
SMEM = pl.BlockSpec(memory_space=pltpu.SMEM)
HBM = pl.BlockSpec(memory_space=pltpu.HBM)
ANY = pl.BlockSpec(memory_space=pl.ANY)


def cost(flops, moved):
    return pl.CostEstimate(flops=flops, bytes_accessed=moved, transcendentals=0)


def room(mib):
    return pltpu.CompilerParams(vmem_limit_bytes=mib << 20)


def shape(dims, dtype):
    return jax.ShapeDtypeStruct(dims, dtype)


def iota(dims, axis):
    return lax.broadcasted_iota(I32, dims, axis)


def scale_rows(scr, key_scales, value_scales):
    scr[...] = jnp.zeros_like(scr)
    scr[0:HELD, 0:KVH] = key_scales[...].astype(F32)
    scr[HELD : 2 * HELD, 0:KVH] = value_scales[...].astype(F32)


def front_kernel(
    dest, slots, keys, values, key_scales, value_scales, hidden, weight, gain,
    message, query, residual,
    held, stage, scr, rows, blocks, in_sem, out_sem, rows_sem, block_sem,
):
    here, rank = lax.axis_index("replica"), lax.axis_index("tensor")
    loads = []
    for j in range(MOVE):
        s = slots[0, j]
        pair = (
            pltpu.make_async_copy(keys.at[s], held.at[j, 0], in_sem.at[j, 0]),
            pltpu.make_async_copy(values.at[s], held.at[j, 1], in_sem.at[j, 1]),
        )
        for copy in pair:
            copy.start()
        loads.append(pair)
    rows_in = pltpu.make_async_copy(hidden, rows, rows_sem)
    rows_in.start()
    depth = blocks.shape[1]
    weights_in = []
    for i in range(STEPS):
        copy = pltpu.make_async_copy(
            weight.at[i * depth : (i + 1) * depth, :], blocks.at[i], block_sem.at[i]
        )
        copy.start()
        weights_in.append(copy)
    scale_rows(scr, key_scales, value_scales)
    row = iota((8, HD), 0)
    stores = []
    for j in range(MOVE):
        s = slots[0, j]
        both = jnp.where(
            row == 0,
            scr[pl.ds(s, 1), :],
            jnp.where(row == 1, scr[pl.ds(HELD + s, 1), :], 0.0),
        )
        stage[j, 2 * KVH * SPAN : SLOT, :] = both.astype(BF16)
        for which in range(2):
            loads[j][which].wait()
            for c in range(KVH):
                at_row = (which * KVH + c) * SPAN
                stage[j, at_row : at_row + SPAN, :] = held[j, which, :, c * HD : (c + 1) * HD]
        copy = pltpu.make_async_copy(stage.at[j], message.at[dest[j, here]], out_sem.at[j])
        copy.start()
        stores.append(copy)
    rows_in.wait()
    total = jnp.zeros((ROWS, 2 * HD), F32)
    for i in range(STEPS):
        weights_in[i].wait()
        total = total + jnp.dot(
            rows[:, i * depth : (i + 1) * depth], blocks[i], preferred_element_type=F32
        )
    for h in range(2):
        part = total[:, h * HD : (h + 1) * HD]
        mean = jnp.mean(part * part, axis=-1, keepdims=True)
        part = part * lax.rsqrt(mean + EPSILON)
        query[:, h * HD : (h + 1) * HD] = (part * gain[...] * HD ** (-0.5)).astype(BF16)
    residual[...] = rows[:, pl.ds(pl.multiple_of(rank * COLS, COLS), COLS)]
    for copy in stores:
        copy.wait()


def front(dest, slots, keys, values, key_scales, value_scales, hidden, q_weight, q_gain):
    depth = hidden.shape[1] // STEPS
    return pl.pallas_call(
        front_kernel,
        out_shape=(
            shape((REPLICAS, SLOT, HD), BF16),
            shape((ROWS, 2 * HD), BF16),
            shape((ROWS, COLS), BF16),
        ),
        in_specs=[SMEM, SMEM, HBM, HBM, VMEM, VMEM, HBM, HBM, VMEM],
        out_specs=(HBM, VMEM, VMEM),
        scratch_shapes=[
            pltpu.VMEM((MOVE, 2, SPAN, KVH * HD), BF16),
            pltpu.VMEM((MOVE, SLOT, HD), BF16),
            pltpu.VMEM((2 * HELD, HD), F32),
            pltpu.VMEM(hidden.shape, BF16),
            pltpu.VMEM((STEPS, depth, 2 * HD), BF16),
            pltpu.SemaphoreType.DMA((MOVE, 2)),
            pltpu.SemaphoreType.DMA((MOVE,)),
            pltpu.SemaphoreType.DMA,
            pltpu.SemaphoreType.DMA((STEPS,)),
        ],
        cost_estimate=cost(1 << 22, 8 << 20),
        compiler_params=room(57),
        name="front",
    )(
        dest, slots, keys, values, key_scales, value_scales, hidden, q_weight,
        q_gain.reshape(1, HD),
    )


def unpack_kernel(
    dest, slots, received, keys, values, key_scales, value_scales,
    new_keys, new_values, new_key_scales, new_value_scales,
    stage, kept, scr, out_sem, kept_sem,
):
    here = lax.axis_index("replica")
    stays = []
    for r in range(HELD):
        moving = slots[0, 0] == r
        for j in range(1, MOVE):
            moving = jnp.logical_or(moving, slots[0, j] == r)
        stays.append(jnp.logical_not(moving))

    def kept_in(r):
        return (
            pltpu.make_async_copy(keys.at[r], kept.at[r, 0], kept_sem.at[r, 0]),
            pltpu.make_async_copy(values.at[r], kept.at[r, 1], kept_sem.at[r, 1]),
        )

    def kept_out(r):
        return (
            pltpu.make_async_copy(kept.at[r, 0], new_keys.at[r], kept_sem.at[r, 0]),
            pltpu.make_async_copy(kept.at[r, 1], new_values.at[r], kept_sem.at[r, 1]),
        )

    for r in range(HELD):

        @pl.when(stays[r])
        def _():
            for copy in kept_in(r):
                copy.start()

    scale_rows(scr, key_scales, value_scales)
    stores = []
    for j in range(MOVE):
        s = slots[0, j]
        source = jnp.int32(0)
        for p in range(REPLICAS):
            source = jnp.where(dest[j, p] == here, p, source)
        both = received[source, 2 * KVH * SPAN : SLOT, :].astype(F32)
        scr[pl.ds(s, 1), :] = both[0:1, :]
        scr[pl.ds(HELD + s, 1), :] = both[1:2, :]
        for which, target in ((0, new_keys), (1, new_values)):
            for c in range(KVH):
                at_row = (which * KVH + c) * SPAN
                stage[j, which, :, c * HD : (c + 1) * HD] = received[
                    source, at_row : at_row + SPAN, :
                ]
            copy = pltpu.make_async_copy(stage.at[j, which], target.at[s], out_sem.at[j, which])
            copy.start()
            stores.append(copy)
    new_key_scales[...] = scr[0:HELD, 0:KVH].astype(BF16)
    new_value_scales[...] = scr[HELD : 2 * HELD, 0:KVH].astype(BF16)
    for r in range(HELD):

        @pl.when(stays[r])
        def _():
            for copy in kept_in(r):
                copy.wait()
            for copy in kept_out(r):
                copy.start()

    for r in range(HELD):

        @pl.when(stays[r])
        def _():
            for copy in kept_out(r):
                copy.wait()

    for copy in stores:
        copy.wait()


def unpack(dest, slots, received, keys, values, key_scales, value_scales):
    return pl.pallas_call(
        unpack_kernel,
        out_shape=(
            shape(keys.shape, BF16),
            shape(values.shape, BF16),
            shape((HELD, KVH), BF16),
            shape((HELD, KVH), BF16),
        ),
        in_specs=[SMEM, SMEM, VMEM, HBM, HBM, VMEM, VMEM],
        out_specs=(HBM, HBM, VMEM, VMEM),
        scratch_shapes=[
            pltpu.VMEM((MOVE, 2, SPAN, KVH * HD), BF16),
            pltpu.VMEM((HELD, 2, SPAN, KVH * HD), BF16),
            pltpu.VMEM((2 * HELD, HD), F32),
            pltpu.SemaphoreType.DMA((MOVE, 2)),
            pltpu.SemaphoreType.DMA((HELD, 2)),
        ],
        cost_estimate=cost(1 << 20, 4 << 20),
        compiler_params=room(8),
        name="unpack",
    )(dest, slots, received, keys, values, key_scales, value_scales)


def split3(x):
    high = x.astype(BF16).astype(F32)
    rest = x - high
    middle = rest.astype(BF16).astype(F32)
    return high, middle, rest - middle


def put_stats(out, at_row, stats):
    high, middle, low = split3(stats)
    out[at_row : at_row + 16, :] = jnp.concatenate([high, middle], axis=0).astype(BF16)
    out[at_row + 16 : at_row + 32, :] = jnp.concatenate(
        [low, jnp.zeros_like(low)], axis=0
    ).astype(BF16)


def get_stats(message, at_row):
    first = message[at_row : at_row + 16, :].astype(F32)
    second = message[at_row + 16 : at_row + 32, :].astype(F32)
    return (first[0:8] + first[8:16]) + second[0:8]


def columns_of(rows):
    short = HD - rows.shape[0]
    return jnp.concatenate([rows, jnp.zeros((short, HD), F32)], axis=0).T


def attend_kernel(
    lengths, q0, q1, q2, q3, keys, values, key_scales, value_scales,
    o0, o1, o2, o3, q_all, o_all, mask, stats,
):
    rank = lax.axis_index("tensor")
    y = rank // 4
    x = (rank // 2) % 2
    for k, q in enumerate((q0, q1, q2, q3)):
        q_all[k] = q[...]
    tokens = HELD * SPAN
    row_request = (iota((HD, tokens), 0) // SPEC) % HELD
    col = iota((HD, tokens), 1)
    limit = jnp.zeros((1, tokens), I32)
    col1 = iota((1, tokens), 1)
    for r in range(HELD):
        limit = jnp.where(col1 // SPAN == r, lengths[r], limit)
    in_reach = rank * SPAN + col1 % SPAN < limit
    ok = jnp.logical_and(row_request == col // SPAN, in_reach)
    mask[...] = jnp.where(ok, 1.0, 0.0)
    spread_cols = (iota((HELD, tokens), 1) // SPAN == iota((HELD, tokens), 0)).astype(BF16)
    spread_rows = ((iota((HD, HELD), 0) // SPEC) % HELD == iota((HD, HELD), 1)).astype(BF16)
    col_scale = lax.dot_general(
        key_scales[...], spread_cols, (((0,), (0,)), ((), ())), preferred_element_type=F32
    )
    row_scale = jnp.dot(spread_rows, value_scales[...], preferred_element_type=F32)
    lane = iota((HD, HD), 1)
    stats[...] = jnp.zeros_like(stats)
    for m in range(KVH):
        k = (y - m // 2 + 4) % 4
        dx = (m % 2 + x) % 2
        near = q_all[k, 2 * dx]
        far = q_all[k, 2 * dx + 1]
        grouped = jnp.concatenate(
            [near[:, :HD], near[:, HD:], far[:, :HD], far[:, HD:]], axis=0
        )
        key = keys[:, :, m * HD : (m + 1) * HD].reshape(tokens, HD)
        value = values[:, :, m * HD : (m + 1) * HD].reshape(tokens, HD)
        scores = lax.dot_general(
            grouped, key, (((1,), (1,)), ((), ())), preferred_element_type=F32
        )
        scores = scores * col_scale[m : m + 1, :]
        good = mask[...] > 0.5
        peak = jnp.max(jnp.where(good, scores, NEGATIVE), axis=1, keepdims=True)
        weight = jnp.where(good, jnp.exp(scores - peak), 0.0)
        total = jnp.sum(weight, axis=1, keepdims=True)
        out = jnp.dot(weight.astype(BF16), value, preferred_element_type=F32)
        o_all[k, dx] = (out * row_scale[:, m : m + 1]).astype(BF16)
        first = 8 * k + 2 * dx
        stats[...] = jnp.where(
            lane == first, peak, jnp.where(lane == first + 1, total, stats[...])
        )
    turned = stats[...].T
    for k, o in enumerate((o0, o1, o2, o3)):
        o[0:HD, :] = o_all[k, 0]
        o[HD : 2 * HD, :] = o_all[k, 1]
        put_stats(o, 2 * HD, turned[8 * k : 8 * k + 8])


def attend(lengths, queries, keys, values, key_scales, value_scales):
    out = shape((2 * HD + 32, HD), BF16)
    return pl.pallas_call(
        attend_kernel,
        out_shape=(out,) * 4,
        in_specs=[SMEM] + [VMEM] * 8,
        out_specs=(VMEM,) * 4,
        scratch_shapes=[
            pltpu.VMEM((4, 4, ROWS, 2 * HD), BF16),
            pltpu.VMEM((4, 2, HD, HD), BF16),
            pltpu.VMEM((HD, HELD * SPAN), F32),
            pltpu.VMEM((HD, HD), F32),
        ],
        cost_estimate=cost(4 << 20, 2 << 20),
        compiler_params=room(8),
        name="attend",
    )(lengths, *queries, keys, values, key_scales, value_scales)


def merged(stats):
    top = functools.reduce(jnp.maximum, stats)
    factors = [jnp.exp(s - top) for s in stats]
    total = sum(s * pltpu.roll(f, 1, 0) for s, f in zip(stats, factors))
    peak_row = iota(top.shape, 0) % 2 == 0
    return factors, jnp.where(peak_row, top, total)


def combine_kernel(p0, p1, p2, p3, o0, o1, o2, o3):
    parts = (p0, p1, p2, p3)
    factors, both = merged([get_stats(p, 2 * HD) for p in parts])
    column = columns_of(jnp.concatenate(factors, axis=0))
    outs = ((o0, o1), (o2, o3))
    for dx in range(2):
        summed = jnp.zeros((HD, HD), F32)
        for k, p in enumerate(parts):
            part = p[dx * HD : (dx + 1) * HD, :].astype(F32)
            summed = summed + part * column[:, 8 * k + 2 * dx : 8 * k + 2 * dx + 1]
        for dc in range(2):
            outs[dx][dc][0 : HD // 2, :] = summed[dc * 64 : dc * 64 + 64].astype(BF16)
            put_stats(outs[dx][dc], HD // 2, both)


def combine(parts):
    out = shape((HD // 2 + 32, HD), BF16)
    return pl.pallas_call(
        combine_kernel,
        out_shape=(out,) * 4,
        in_specs=[VMEM] * 4,
        out_specs=(VMEM,) * 4,
        cost_estimate=cost(1 << 20, 1 << 19),
        compiler_params=room(4),
        name="combine",
    )(*parts)


def finished(parts):
    stats = []
    for d, p in enumerate(parts):
        s = get_stats(p, HD // 2)
        if d // 2:
            s = pltpu.roll(s, 6, 0)
        if d % 2:
            s = pltpu.roll(s, HD // 2, 1)
        stats.append(s)
    factors, both = merged(stats)
    over = pltpu.roll(both, 7, 0)
    column = columns_of(jnp.concatenate([f / over for f in factors], axis=0))
    summed = jnp.zeros((HD // 2, HD), F32)
    for d, p in enumerate(parts):
        summed = summed + p[0 : HD // 2, :].astype(F32) * column[0 : HD // 2, 8 * d : 8 * d + 1]
    return summed.astype(BF16)


def half_in(core, weight, blocks, sem):
    copies = []
    for i in range(TENSORS // 2):
        start = pl.multiple_of((2 * i + core) * COLS, COLS)
        copy = pltpu.make_async_copy(weight.at[:, pl.ds(start, COLS)], blocks.at[i], sem.at[i])
        copy.start()
        copies.append(copy)
    return copies


def half_out(copies, attended, blocks, out):
    for i, copy in enumerate(copies):
        copy.wait()
        out[i] = jnp.dot(attended, blocks[i], preferred_element_type=F32).astype(out.dtype)


def output_other_kernel(p0, p1, p2, p3, weight, attended, out, blocks, sem):
    copies = half_in(1 - lax.axis_index("tensor") % 2, weight, blocks, sem)
    both = finished((p0, p1, p2, p3))
    for h in range(2):
        attended[:, h * HD : (h + 1) * HD] = both[h * ROWS : (h + 1) * ROWS]
    half_out(copies, attended[...], blocks, out)


def output_own_kernel(attended, weight, out, blocks, sem):
    copies = half_in(lax.axis_index("tensor") % 2, weight, blocks, sem)
    half_out(copies, attended[...], blocks, out)


HALF_SCRATCH = [
    pltpu.VMEM((TENSORS // 2, 2 * HD, COLS), BF16),
    pltpu.SemaphoreType.DMA((TENSORS // 2,)),
]


def output_other(parts, o_weight):
    return pl.pallas_call(
        output_other_kernel,
        out_shape=(
            shape((ROWS, 2 * HD), BF16),
            shape((TENSORS // 2, ROWS, COLS), BF16),
        ),
        in_specs=[VMEM] * 4 + [ANY],
        out_specs=(VMEM, VMEM),
        scratch_shapes=HALF_SCRATCH,
        cost_estimate=cost(1 << 22, 2 << 20),
        compiler_params=room(51),
        name="output_other",
    )(*parts, o_weight)


def output_own(attended, o_weight):
    return pl.pallas_call(
        output_own_kernel,
        out_shape=shape((TENSORS // 2, ROWS, COLS), F32),
        in_specs=[VMEM, ANY],
        out_specs=VMEM,
        scratch_shapes=HALF_SCRATCH,
        cost_estimate=cost(1 << 22, 2 << 20),
        compiler_params=room(51),
        name="output_own",
    )(attended, o_weight)


def share_kernel(own, received, keep, s1, s2, s3):
    y = lax.axis_index("tensor") // 4
    for k in range(4):
        group = (y - k + 4) % 4
        for c in range(2):
            value = own[2 * group + c] + received[2 * group + c].astype(F32)
            if k == 0:
                keep[c] = value
            else:
                (s1, s2, s3)[k - 1][c] = value.astype(BF16)


def share(own, received):
    out = shape((2, ROWS, COLS), BF16)
    return pl.pallas_call(
        share_kernel,
        out_shape=(shape((2, ROWS, COLS), F32), out, out, out),
        in_specs=[VMEM, VMEM],
        out_specs=(VMEM,) * 4,
        cost_estimate=cost(1 << 20, 1 << 20),
        compiler_params=room(6),
        name="share",
    )(own, received)


def narrow_kernel(own, r1, r2, r3, keep, send):
    x = (lax.axis_index("tensor") // 2) % 2
    for c, out in ((x, keep), (1 - x, send)):
        value = own[c] + r1[c].astype(F32) + r2[c].astype(F32) + r3[c].astype(F32)
        out[...] = value.astype(out.dtype)


def narrow(own, received):
    return pl.pallas_call(
        narrow_kernel,
        out_shape=(shape((ROWS, COLS), F32), shape((ROWS, COLS), BF16)),
        in_specs=[VMEM] * 4,
        out_specs=(VMEM,) * 2,
        cost_estimate=cost(1 << 20, 1 << 19),
        compiler_params=room(4),
        name="narrow",
    )(own, *received)


def mix_kernel(gate, own, received, residual, out):
    scale = jnp.tanh(jnp.full((8, HD), gate[0], F32))[0:1, 0:1]
    summed = own[...] + received[...].astype(F32)
    out[...] = (residual[...].astype(F32) + scale * summed).astype(BF16)


def mix(gate, own, received, residual):
    return pl.pallas_call(
        mix_kernel,
        out_shape=shape((ROWS, COLS), BF16),
        in_specs=[SMEM, VMEM, VMEM, VMEM],
        out_specs=VMEM,
        cost_estimate=cost(1 << 20, 1 << 18),
        compiler_params=room(4),
        name="mix",
    )(gate, own, received, residual)


def swap(array, bits):
    return lax.ppermute(array, "tensor", [(i, i ^ bits) for i in range(TENSORS)])


def shift(array, rows):
    return lax.ppermute(array, "tensor", [(i, (i + 4 * rows) % TENSORS) for i in range(TENSORS)])


def attention(
    query, residual, o_weight, attn_gate, keys, values, key_scales, value_scales, lengths
):
    local = jnp.stack([query] + [swap(query, d) for d in (1, 2, 3)])
    queries = [local] + [shift(local, k) for k in (1, 2, 3)]
    parts = attend(lengths, queries, keys, values, key_scales, value_scales)
    parts = combine([parts[0]] + [shift(parts[k], -k) for k in (1, 2, 3)])
    parts = [parts[0]] + [swap(parts[d], d) for d in (1, 2, 3)]
    attended, other = output_other(parts, o_weight)
    other = swap(other, 1)
    own, *sent = share(output_own(attended, o_weight), other)
    own, sent = narrow(own, [shift(s, -k) for k, s in zip((1, 2, 3), sent)])
    return mix(attn_gate, own, swap(sent, 2), residual)


def local(
    hidden,
    q_weight,
    q_gain,
    o_weight,
    attn_gate,
    key_codes,
    value_codes,
    key_scales,
    value_scales,
    lengths,
    dest_replica,
    move_slot,
):
    dest = dest_replica.T
    key_scales, value_scales = key_scales[:, 0, :], value_scales[:, 0, :]
    message, query, residual = front(
        dest, move_slot, key_codes, value_codes, key_scales, value_scales,
        hidden, q_weight, q_gain,
    )
    received = lax.all_to_all(
        message, "replica", split_axis=0, concat_axis=0, tiled=True
    )
    mixed = attention(
        query, residual, o_weight, attn_gate,
        key_codes, value_codes, key_scales, value_scales, lengths,
    )
    new_keys, new_values, new_ks, new_vs = unpack(
        dest, move_slot, received, key_codes, value_codes, key_scales, value_scales
    )
    return (mixed, new_keys, new_values, new_ks[:, None, :], new_vs[:, None, :])


def solution(mesh):
    return jax.shard_map(
        local,
        mesh=mesh,
        in_specs=(
            P("replica", None),
            P(None, "tensor"),
            P(),
            P("tensor", None),
            P(),
            P("replica", "tensor", None),
            P("replica", "tensor", None),
            P("replica", "tensor", None),
            P("replica", "tensor", None),
            P("replica"),
            P(),
            P("replica", None),
        ),
        out_specs=(
            P("replica", "tensor"),
            P("replica", "tensor", None),
            P("replica", "tensor", None),
            P("replica", "tensor", None),
            P("replica", "tensor", None),
        ),
        check_vma=False,
    )
```

```python
import functools

import jax
import jax.numpy as jnp
from jax import lax
from jax.experimental import pallas as pl
from jax.experimental.pallas import tpu as pltpu
from jax.sharding import PartitionSpec as P

NEGATIVE = -1e30
EPSILON = 1e-06
BF16, F32, I32 = jnp.bfloat16, jnp.float32, jnp.int32

REPLICAS = 16
MOVE = 6
HELD = 8
SPAN = 32
SPEC = 4
ROWS = HELD * SPEC
KVH = 8
HD = 128
TENSORS = 16
SLOT = 2 * KVH * SPAN + 8
COLS = 512
STEPS = 8
FRONT_ROOM, QUERY_ROOM, OUTPUT_ROOM = 57, 53.6, 51


VMEM = pl.BlockSpec(memory_space=pltpu.VMEM)
SMEM = pl.BlockSpec(memory_space=pltpu.SMEM)
HBM = pl.BlockSpec(memory_space=pltpu.HBM)
ANY = pl.BlockSpec(memory_space=pl.ANY)


def cost(flops, moved):
    return pl.CostEstimate(flops=flops, bytes_accessed=moved, transcendentals=0)


def room(mib):
    return pltpu.CompilerParams(vmem_limit_bytes=int(mib * (1 << 20)))


def shape(dims, dtype):
    return jax.ShapeDtypeStruct(dims, dtype)


def iota(dims, axis):
    return lax.broadcasted_iota(I32, dims, axis)


def scale_rows(scr, key_scales, value_scales):
    scr[...] = jnp.zeros_like(scr)
    scr[0:HELD, 0:KVH] = key_scales[...].astype(F32)
    scr[HELD : 2 * HELD, 0:KVH] = value_scales[...].astype(F32)


def front_kernel(
    dest, slots, keys, values, key_scales, value_scales,
    message, other, plan,
    held, stage, scr, in_sem, out_sem,
):
    here = lax.axis_index("replica")
    x = (lax.axis_index("tensor") // 2) % 2
    loads = []
    for r in range(HELD):
        pair = (
            pltpu.make_async_copy(keys.at[r], held.at[r, 0], in_sem.at[r, 0]),
            pltpu.make_async_copy(values.at[r], held.at[r, 1], in_sem.at[r, 1]),
        )
        for copy in pair:
            copy.start()
        loads.append(pair)
    scale_rows(scr, key_scales, value_scales)
    for r in range(HELD):
        plan[r] = -1
    for j in range(MOVE):
        source = jnp.int32(0)
        for p in range(REPLICAS):
            source = jnp.where(dest[j, p] == here, p, source)
        plan[slots[0, j]] = source
    row = iota((8, HD), 0)
    for pair in loads:
        for copy in pair:
            copy.wait()
    stores = []
    for j in range(MOVE):
        s = slots[0, j]
        both = jnp.where(
            row == 0,
            scr[pl.ds(s, 1), :],
            jnp.where(row == 1, scr[pl.ds(HELD + s, 1), :], 0.0),
        )
        stage[j, 2 * KVH * SPAN : SLOT, :] = both.astype(BF16)
        for which in range(2):
            for c in range(KVH):
                at_row = (which * KVH + c) * SPAN
                stage[j, at_row : at_row + SPAN, :] = held[s, which, :, c * HD : (c + 1) * HD]
        copy = pltpu.make_async_copy(stage.at[j], message.at[dest[j, here]], out_sem.at[j])
        copy.start()
        stores.append(copy)
    for i in range(KVH // 2):
        start = pl.multiple_of((2 * i + 1 - x) * HD, HD)
        for which in range(2):
            for r in range(HELD):
                at_row = (which * HELD + r) * SPAN
                other[at_row : at_row + SPAN, i * HD : (i + 1) * HD] = held[
                    r, which, :, pl.ds(start, HD)
                ]
    other[2 * HELD * SPAN :, 0:HD] = scr[...].astype(BF16)
    other[2 * HELD * SPAN :, HD:] = jnp.zeros((2 * HELD, 3 * HD), BF16)
    for copy in stores:
        copy.wait()


def front(dest, slots, keys, values, key_scales, value_scales):
    return pl.pallas_call(
        front_kernel,
        out_shape=(
            shape((REPLICAS, SLOT, HD), BF16),
            shape((2 * HELD * SPAN + 2 * HELD, KVH // 2 * HD), BF16),
            shape((HELD,), I32),
        ),
        in_specs=[SMEM, SMEM, HBM, HBM, VMEM, VMEM],
        out_specs=(HBM, VMEM, SMEM),
        scratch_shapes=[
            pltpu.VMEM((HELD, 2, SPAN, KVH * HD), BF16),
            pltpu.VMEM((MOVE, SLOT, HD), BF16),
            pltpu.VMEM((2 * HELD, HD), F32),
            pltpu.SemaphoreType.DMA((HELD, 2)),
            pltpu.SemaphoreType.DMA((MOVE,)),
        ],
        cost_estimate=cost(1 << 20, 4 << 20),
        compiler_params=room(FRONT_ROOM),
        name="front",
    )(dest, slots, keys, values, key_scales, value_scales)


def unpack_kernel(
    plan, received, keys, values, key_scales, value_scales,
    new_keys, new_values, new_key_scales, new_value_scales,
    stage, scr, in_sem, out_sem,
):
    def copies(r, inward):
        pairs = ((keys, new_keys), (values, new_values))
        if inward:
            return [
                pltpu.make_async_copy(old.at[r], stage.at[r, i], in_sem.at[r, i])
                for i, (old, _) in enumerate(pairs)
            ]
        return [
            pltpu.make_async_copy(stage.at[r, i], new.at[r], out_sem.at[r, i])
            for i, (_, new) in enumerate(pairs)
        ]

    for r in range(HELD):

        @pl.when(plan[r] < 0)
        def _():
            for copy in copies(r, True):
                copy.start()

    scale_rows(scr, key_scales, value_scales)
    for r in range(HELD):
        source = plan[r]

        @pl.when(source >= 0)
        def _():
            both = received[source, 2 * KVH * SPAN : SLOT, :].astype(F32)
            scr[r : r + 1, :] = both[0:1, :]
            scr[HELD + r : HELD + r + 1, :] = both[1:2, :]
            for which in range(2):
                for c in range(KVH):
                    at_row = (which * KVH + c) * SPAN
                    stage[r, which, :, c * HD : (c + 1) * HD] = received[
                        source, at_row : at_row + SPAN, :
                    ]
            for copy in copies(r, False):
                copy.start()

    for r in range(HELD):

        @pl.when(plan[r] < 0)
        def _():
            for copy in copies(r, True):
                copy.wait()
            for copy in copies(r, False):
                copy.start()

    new_key_scales[...] = scr[0:HELD, 0:KVH].astype(BF16)
    new_value_scales[...] = scr[HELD : 2 * HELD, 0:KVH].astype(BF16)
    for r in range(HELD):
        for copy in copies(r, False):
            copy.wait()


def unpack(plan, received, keys, values, key_scales, value_scales):
    return pl.pallas_call(
        unpack_kernel,
        out_shape=(
            shape(keys.shape, BF16),
            shape(values.shape, BF16),
            shape((HELD, KVH), BF16),
            shape((HELD, KVH), BF16),
        ),
        in_specs=[SMEM, VMEM, HBM, HBM, VMEM, VMEM],
        out_specs=(HBM, HBM, VMEM, VMEM),
        scratch_shapes=[
            pltpu.VMEM((HELD, 2, SPAN, KVH * HD), BF16),
            pltpu.VMEM((2 * HELD, HD), F32),
            pltpu.SemaphoreType.DMA((HELD, 2)),
            pltpu.SemaphoreType.DMA((HELD, 2)),
        ],
        cost_estimate=cost(1 << 20, 4 << 20),
        compiler_params=room(8),
        name="unpack",
    )(plan, received, keys, values, key_scales, value_scales)


def query_kernel(hidden, weight, gain, query, residual, rows, blocks, rows_sem, block_sem):
    rank = lax.axis_index("tensor")
    depth = blocks.shape[1]
    rows_in = pltpu.make_async_copy(hidden, rows, rows_sem)
    rows_in.start()
    weights_in = []
    for i in range(STEPS):
        copy = pltpu.make_async_copy(
            weight.at[i * depth : (i + 1) * depth, :], blocks.at[i], block_sem.at[i]
        )
        copy.start()
        weights_in.append(copy)
    rows_in.wait()
    residual[...] = rows[:, pl.ds(pl.multiple_of(rank * COLS, COLS), COLS)]
    total = jnp.zeros((ROWS, 2 * HD), F32)
    for i in range(STEPS):
        weights_in[i].wait()
        total = total + jnp.dot(
            rows[:, i * depth : (i + 1) * depth], blocks[i], preferred_element_type=F32
        )
    for h in range(2):
        part = total[:, h * HD : (h + 1) * HD]
        mean = jnp.mean(part * part, axis=-1, keepdims=True)
        part = part * lax.rsqrt(mean + EPSILON)
        query[:, h * HD : (h + 1) * HD] = (part * gain[...] * HD ** (-0.5)).astype(BF16)


def project_query(hidden, q_weight, q_gain):
    depth = hidden.shape[1] // STEPS
    return pl.pallas_call(
        query_kernel,
        out_shape=(shape((ROWS, 2 * HD), BF16), shape((ROWS, COLS), BF16)),
        in_specs=[HBM, HBM, VMEM],
        out_specs=(VMEM, VMEM),
        scratch_shapes=[
            pltpu.VMEM(hidden.shape, BF16),
            pltpu.VMEM((STEPS, depth, 2 * HD), BF16),
            pltpu.SemaphoreType.DMA,
            pltpu.SemaphoreType.DMA((STEPS,)),
        ],
        cost_estimate=cost(1 << 22, 5 << 20),
        compiler_params=room(QUERY_ROOM),
        name="query",
    )(hidden, q_weight, q_gain.reshape(1, HD))


def split3(x):
    high = x.astype(BF16).astype(F32)
    rest = x - high
    middle = rest.astype(BF16).astype(F32)
    return high, middle, rest - middle


def put_stats(out, at_row, stats):
    high, middle, low = split3(stats)
    out[at_row : at_row + 16, :] = jnp.concatenate([high, middle], axis=0).astype(BF16)
    out[at_row + 16 : at_row + 32, :] = jnp.concatenate(
        [low, jnp.zeros_like(low)], axis=0
    ).astype(BF16)


def get_stats(message, at_row):
    first = message[at_row : at_row + 16, :].astype(F32)
    second = message[at_row + 16 : at_row + 32, :].astype(F32)
    return (first[0:8] + first[8:16]) + second[0:8]


def columns_of(rows):
    short = HD - rows.shape[0]
    return jnp.concatenate([rows, jnp.zeros((short, HD), F32)], axis=0).T


def attend_kernel(
    lengths, q0, q1, q2, q3, keys, values, key_scales, value_scales, other,
    o0, o1, o2, o3, q_all, o_all, mask, stats,
):
    rank = lax.axis_index("tensor")
    y = rank // 4
    x = (rank // 2) % 2
    for k, q in enumerate((q0, q1, q2, q3)):
        q_all[k] = q[...]
    tokens = HELD * SPAN
    row_request = (iota((HD, tokens), 0) // SPEC) % HELD
    col = iota((HD, tokens), 1)
    limit = jnp.zeros((1, tokens), I32)
    col1 = iota((1, tokens), 1)
    for r in range(HELD):
        limit = jnp.where(col1 // SPAN == r, lengths[r], limit)
    own_request = row_request == col // SPAN
    beside = rank + 2 - 4 * x
    for b, block in enumerate((rank, beside)):
        in_reach = block * SPAN + col1 % SPAN < limit
        mask[b] = jnp.where(jnp.logical_and(own_request, in_reach), 1.0, 0.0)
    spread_cols = (iota((HELD, tokens), 1) // SPAN == iota((HELD, tokens), 0)).astype(BF16)
    spread_rows = ((iota((HD, HELD), 0) // SPEC) % HELD == iota((HD, HELD), 1)).astype(BF16)
    end = 2 * tokens
    scales = (
        (key_scales[...], value_scales[...]),
        (other[end : end + HELD, 0:KVH], other[end + HELD : end + 2 * HELD, 0:KVH]),
    )
    col_scale = [
        lax.dot_general(
            k, spread_cols, (((0,), (0,)), ((), ())), preferred_element_type=F32
        )
        for k, _ in scales
    ]
    row_scale = [jnp.dot(spread_rows, v, preferred_element_type=F32) for _, v in scales]
    lane = iota((HD, HD), 1)
    stats[...] = jnp.zeros_like(stats)
    for i in range(KVH // 2):
        k = (y - i + 4) % 4
        near, far = q_all[k, 0], q_all[k, 1]
        grouped = jnp.concatenate(
            [near[:, :HD], near[:, HD:], far[:, :HD], far[:, HD:]], axis=0
        )
        start = pl.multiple_of((2 * i + x) * HD, HD)
        lanes = slice(i * HD, (i + 1) * HD)
        key = (keys[:, :, pl.ds(start, HD)].reshape(tokens, HD), other[0:tokens, lanes])
        value = (
            values[:, :, pl.ds(start, HD)].reshape(tokens, HD),
            other[tokens : 2 * tokens, lanes],
        )
        scores, peaks = [], []
        for b in range(2):
            across = jnp.where(
                x == 0, col_scale[b][2 * i : 2 * i + 1], col_scale[b][2 * i + 1 : 2 * i + 2]
            )
            score = across * lax.dot_general(
                grouped, key[b], (((1,), (1,)), ((), ())), preferred_element_type=F32
            )
            scores.append(score)
            masked = jnp.where(mask[b] > 0.5, score, NEGATIVE)
            peaks.append(jnp.max(masked, axis=1, keepdims=True))
        peak = jnp.maximum(*peaks)
        total, out = 0.0, 0.0
        for b in range(2):
            weight = jnp.where(mask[b] > 0.5, jnp.exp(scores[b] - peak), 0.0)
            total = total + jnp.sum(weight, axis=1, keepdims=True)
            down = jnp.where(
                x == 0, row_scale[b][:, 2 * i : 2 * i + 1], row_scale[b][:, 2 * i + 1 : 2 * i + 2]
            )
            out = out + down * jnp.dot(
                weight.astype(BF16), value[b], preferred_element_type=F32
            )
        o_all[k] = out.astype(BF16)
        stats[...] = jnp.where(
            lane == 8 * k, peak, jnp.where(lane == 8 * k + 1, total, stats[...])
        )
    turned = stats[...].T
    for k, o in enumerate((o0, o1, o2, o3)):
        o[0:HD, :] = o_all[k]
        put_stats(o, HD, turned[8 * k : 8 * k + 8])


def attend(lengths, queries, keys, values, key_scales, value_scales, other):
    out = shape((HD + 32, HD), BF16)
    return pl.pallas_call(
        attend_kernel,
        out_shape=(out,) * 4,
        in_specs=[SMEM] + [VMEM] * 9,
        out_specs=(VMEM,) * 4,
        scratch_shapes=[
            pltpu.VMEM((4, 2, ROWS, 2 * HD), BF16),
            pltpu.VMEM((4, HD, HD), BF16),
            pltpu.VMEM((2, HD, HELD * SPAN), F32),
            pltpu.VMEM((HD, HD), F32),
        ],
        cost_estimate=cost(4 << 20, 2 << 20),
        compiler_params=room(8),
        name="attend",
    )(lengths, *queries, keys, values, key_scales, value_scales, other)


def merged(stats):
    top = functools.reduce(jnp.maximum, stats)
    factors = [jnp.exp(s - top) for s in stats]
    total = sum(s * pltpu.roll(f, 1, 0) for s, f in zip(stats, factors))
    peak_row = iota(top.shape, 0) % 2 == 0
    return factors, jnp.where(peak_row, top, total)


def combine_kernel(p0, p1, p2, p3, o0, o1):
    parts = (p0, p1, p2, p3)
    factors, both = merged([get_stats(p, HD) for p in parts])
    column = columns_of(jnp.concatenate(factors, axis=0))
    summed = jnp.zeros((HD, HD), F32)
    for k, p in enumerate(parts):
        summed = summed + p[0:HD, :].astype(F32) * column[:, 8 * k : 8 * k + 1]
    for dc, o in enumerate((o0, o1)):
        o[0 : HD // 2, :] = summed[dc * 64 : dc * 64 + 64].astype(BF16)
        put_stats(o, HD // 2, both)


def combine(parts):
    out = shape((HD // 2 + 32, HD), BF16)
    return pl.pallas_call(
        combine_kernel,
        out_shape=(out,) * 2,
        in_specs=[VMEM] * 4,
        out_specs=(VMEM,) * 2,
        cost_estimate=cost(1 << 20, 1 << 19),
        compiler_params=room(4),
        name="combine",
    )(*parts)


def finished(parts):
    stats = []
    for d, p in enumerate(parts):
        s = get_stats(p, HD // 2)
        stats.append(pltpu.roll(s, HD // 2, 1) if d else s)
    factors, both = merged(stats)
    over = pltpu.roll(both, 7, 0)
    column = columns_of(jnp.concatenate([f / over for f in factors], axis=0))
    summed = jnp.zeros((HD // 2, HD), F32)
    for d, p in enumerate(parts):
        summed = summed + p[0 : HD // 2, :].astype(F32) * column[0 : HD // 2, 8 * d : 8 * d + 1]
    return summed.astype(BF16)


def half_in(core, weight, blocks, sem):
    copies = []
    for i in range(TENSORS // 2):
        start = pl.multiple_of((2 * i + core) * COLS, COLS)
        copy = pltpu.make_async_copy(weight.at[:, pl.ds(start, COLS)], blocks.at[i], sem.at[i])
        copy.start()
        copies.append(copy)
    return copies


def half_out(copies, attended, blocks, out):
    for i, copy in enumerate(copies):
        copy.wait()
        out[i] = jnp.dot(attended, blocks[i], preferred_element_type=F32).astype(out.dtype)


def output_other_kernel(p0, p1, weight, attended, out, blocks, sem):
    copies = half_in(1 - lax.axis_index("tensor") % 2, weight, blocks, sem)
    both = finished((p0, p1))
    for h in range(2):
        attended[:, h * HD : (h + 1) * HD] = both[h * ROWS : (h + 1) * ROWS]
    half_out(copies, attended[...], blocks, out)


def output_own_kernel(attended, weight, out, blocks, sem):
    copies = half_in(lax.axis_index("tensor") % 2, weight, blocks, sem)
    half_out(copies, attended[...], blocks, out)


HALF_SCRATCH = [
    pltpu.VMEM((TENSORS // 2, 2 * HD, COLS), BF16),
    pltpu.SemaphoreType.DMA((TENSORS // 2,)),
]


def output_other(parts, o_weight):
    return pl.pallas_call(
        output_other_kernel,
        out_shape=(
            shape((ROWS, 2 * HD), BF16),
            shape((TENSORS // 2, ROWS, COLS), BF16),
        ),
        in_specs=[VMEM] * 2 + [ANY],
        out_specs=(VMEM, VMEM),
        scratch_shapes=HALF_SCRATCH,
        cost_estimate=cost(1 << 22, 2 << 20),
        compiler_params=room(OUTPUT_ROOM),
        name="output_other",
    )(*parts, o_weight)


def output_own(attended, o_weight):
    return pl.pallas_call(
        output_own_kernel,
        out_shape=shape((TENSORS // 2, ROWS, COLS), F32),
        in_specs=[VMEM, ANY],
        out_specs=VMEM,
        scratch_shapes=HALF_SCRATCH,
        cost_estimate=cost(1 << 22, 2 << 20),
        compiler_params=room(OUTPUT_ROOM),
        name="output_own",
    )(attended, o_weight)


def share_kernel(own, received, keep, s1, s2, s3):
    y = lax.axis_index("tensor") // 4
    for k in range(4):
        group = (y - k + 4) % 4
        for c in range(2):
            value = own[2 * group + c] + received[2 * group + c].astype(F32)
            if k == 0:
                keep[c] = value
            else:
                (s1, s2, s3)[k - 1][c] = value.astype(BF16)


def share(own, received):
    out = shape((2, ROWS, COLS), BF16)
    return pl.pallas_call(
        share_kernel,
        out_shape=(shape((2, ROWS, COLS), F32), out, out, out),
        in_specs=[VMEM, VMEM],
        out_specs=(VMEM,) * 4,
        cost_estimate=cost(1 << 20, 1 << 20),
        compiler_params=room(6),
        name="share",
    )(own, received)


def narrow_kernel(own, r1, r2, r3, keep, send):
    x = (lax.axis_index("tensor") // 2) % 2
    for c, out in ((x, keep), (1 - x, send)):
        value = own[c] + r1[c].astype(F32) + r2[c].astype(F32) + r3[c].astype(F32)
        out[...] = value.astype(out.dtype)


def narrow(own, received):
    return pl.pallas_call(
        narrow_kernel,
        out_shape=(shape((ROWS, COLS), F32), shape((ROWS, COLS), BF16)),
        in_specs=[VMEM] * 4,
        out_specs=(VMEM,) * 2,
        cost_estimate=cost(1 << 20, 1 << 19),
        compiler_params=room(4),
        name="narrow",
    )(own, *received)


def mix_kernel(gate, own, received, residual, out):
    scale = jnp.tanh(jnp.full((8, HD), gate[0], F32))[0:1, 0:1]
    summed = own[...] + received[...].astype(F32)
    out[...] = (residual[...].astype(F32) + scale * summed).astype(BF16)


def mix(gate, own, received, residual):
    return pl.pallas_call(
        mix_kernel,
        out_shape=shape((ROWS, COLS), BF16),
        in_specs=[SMEM, VMEM, VMEM, VMEM],
        out_specs=VMEM,
        cost_estimate=cost(1 << 20, 1 << 18),
        compiler_params=room(4),
        name="mix",
    )(gate, own, received, residual)


def swap(array, bits):
    return lax.ppermute(array, "tensor", [(i, i ^ bits) for i in range(TENSORS)])


def shift(array, rows):
    return lax.ppermute(array, "tensor", [(i, (i + 4 * rows) % TENSORS) for i in range(TENSORS)])


def attention(
    hidden, q_weight, q_gain, o_weight, attn_gate,
    keys, values, key_scales, value_scales, other, lengths,
):
    query, residual = project_query(hidden, q_weight, q_gain)
    local = jnp.stack([query, swap(query, 1)])
    queries = [local] + [shift(local, k) for k in (1, 2, 3)]
    parts = attend(lengths, queries, keys, values, key_scales, value_scales, other)
    parts = combine([parts[0]] + [shift(parts[k], -k) for k in (1, 2, 3)])
    attended, sent = output_other([parts[0], swap(parts[1], 1)], o_weight)
    sent = swap(sent, 1)
    own, *sent = share(output_own(attended, o_weight), sent)
    own, sent = narrow(own, [shift(s, -k) for k, s in zip((1, 2, 3), sent)])
    return mix(attn_gate, own, swap(sent, 2), residual)


def local(
    hidden,
    q_weight,
    q_gain,
    o_weight,
    attn_gate,
    key_codes,
    value_codes,
    key_scales,
    value_scales,
    lengths,
    dest_replica,
    move_slot,
):
    dest = dest_replica.T
    key_scales, value_scales = key_scales[:, 0, :], value_scales[:, 0, :]
    message, other, plan = front(dest, move_slot, key_codes, value_codes, key_scales, value_scales)
    other = swap(other, 2)
    received = lax.all_to_all(
        message, "replica", split_axis=0, concat_axis=0, tiled=True
    )
    mixed = attention(
        hidden, q_weight, q_gain, o_weight, attn_gate,
        key_codes, value_codes, key_scales, value_scales, other, lengths,
    )
    new_keys, new_values, new_ks, new_vs = unpack(
        plan, received, key_codes, value_codes, key_scales, value_scales
    )
    return (mixed, new_keys, new_values, new_ks[:, None, :], new_vs[:, None, :])


def solution(mesh):
    return jax.shard_map(
        local,
        mesh=mesh,
        in_specs=(
            P("replica", None),
            P(None, "tensor"),
            P(),
            P("tensor", None),
            P(),
            P("replica", "tensor", None),
            P("replica", "tensor", None),
            P("replica", "tensor", None),
            P("replica", "tensor", None),
            P("replica"),
            P(),
            P("replica", None),
        ),
        out_specs=(
            P("replica", "tensor"),
            P("replica", "tensor", None),
            P("replica", "tensor", None),
            P("replica", "tensor", None),
            P("replica", "tensor", None),
        ),
        check_vma=False,
    )
```

```python
import functools

import jax
import jax.numpy as jnp
from jax import lax
from jax.experimental import pallas as pl
from jax.experimental.pallas import tpu as pltpu
from jax.sharding import PartitionSpec as P

NEGATIVE = -1e30
EPSILON = 1e-06
BF16, F32, I32 = jnp.bfloat16, jnp.float32, jnp.int32

REPLICAS = 16
MOVE = 6
HELD = 8
SPAN = 32
SPEC = 4
ROWS = HELD * SPEC
KVH = 8
HD = 128
TENSORS = 16
SLOT = 2 * KVH * SPAN + 8
COLS = 512
STEPS = 8
FRONT_ROOM, QUERY_ROOM, OUTPUT_ROOM = 57, 53.6, 51


VMEM = pl.BlockSpec(memory_space=pltpu.VMEM)
SMEM = pl.BlockSpec(memory_space=pltpu.SMEM)
HBM = pl.BlockSpec(memory_space=pltpu.HBM)
ANY = pl.BlockSpec(memory_space=pl.ANY)


def cost(flops, moved):
    return pl.CostEstimate(flops=flops, bytes_accessed=moved, transcendentals=0)


def room(mib):
    return pltpu.CompilerParams(vmem_limit_bytes=int(mib * (1 << 20)))


def shape(dims, dtype):
    return jax.ShapeDtypeStruct(dims, dtype)


def iota(dims, axis):
    return lax.broadcasted_iota(I32, dims, axis)


def scale_rows(scr, key_scales, value_scales):
    scr[...] = jnp.zeros_like(scr)
    scr[0:HELD, 0:KVH] = key_scales[...].astype(F32)
    scr[HELD : 2 * HELD, 0:KVH] = value_scales[...].astype(F32)


def front_kernel(
    dest_in, slots_in, keys, values, key_scales_in, value_scales_in,
    message, other_out, plan_out,
    dest, slots, plan, scales, held, stage, other, scr,
    small_sem, in_sem, out_sem, end_sem,
):
    here = lax.axis_index("replica")
    x = (lax.axis_index("tensor") // 2) % 2
    small = [
        pltpu.make_async_copy(source, target, small_sem.at[i])
        for i, (source, target) in enumerate(
            (
                (slots_in, slots),
                (dest_in, dest),
                (key_scales_in, scales.at[0]),
                (value_scales_in, scales.at[1]),
            )
        )
    ]
    for copy in small:
        copy.start()

    def loads(r):
        return (
            pltpu.make_async_copy(keys.at[r], held.at[r, 0], in_sem.at[r, 0]),
            pltpu.make_async_copy(values.at[r], held.at[r, 1], in_sem.at[r, 1]),
        )

    for r in range(HELD):
        for copy in loads(r):
            copy.start()
    for copy in small:
        copy.wait()
    for r in range(HELD):
        plan[r] = -1
    for j in range(MOVE):
        source = jnp.int32(0)
        for p in range(REPLICAS):
            source = jnp.where(dest[j, p] == here, p, source)
        plan[slots[0, j]] = source
    plan_copy = pltpu.make_async_copy(plan, plan_out, end_sem.at[0])
    plan_copy.start()
    scale_rows(scr, scales.at[0], scales.at[1])
    row = iota((8, HD), 0)
    for r in range(HELD):
        for copy in loads(r):
            copy.wait()
    stores = []
    for j in range(MOVE):
        s = slots[0, j]
        both = jnp.where(
            row == 0,
            scr[pl.ds(s, 1), :],
            jnp.where(row == 1, scr[pl.ds(HELD + s, 1), :], 0.0),
        )
        stage[j, 2 * KVH * SPAN : SLOT, :] = both.astype(BF16)
        for which in range(2):
            for c in range(KVH):
                at_row = (which * KVH + c) * SPAN
                stage[j, at_row : at_row + SPAN, :] = held[s, which, :, c * HD : (c + 1) * HD]
        copy = pltpu.make_async_copy(stage.at[j], message.at[dest[j, here]], out_sem.at[j])
        copy.start()
        stores.append(copy)
    for i in range(KVH // 2):
        start = pl.multiple_of((2 * i + 1 - x) * HD, HD)
        for which in range(2):
            for r in range(HELD):
                at_row = (which * HELD + r) * SPAN
                other[at_row : at_row + SPAN, i * HD : (i + 1) * HD] = held[
                    r, which, :, pl.ds(start, HD)
                ]
    other[2 * HELD * SPAN :, 0:HD] = scr[...].astype(BF16)
    other[2 * HELD * SPAN :, HD:] = jnp.zeros((2 * HELD, 3 * HD), BF16)
    other_copy = pltpu.make_async_copy(other, other_out, end_sem.at[1])
    other_copy.start()
    for copy in stores:
        copy.wait()
    plan_copy.wait()
    other_copy.wait()


def front(dest, slots, keys, values, key_scales, value_scales):
    other = (2 * HELD * SPAN + 2 * HELD, KVH // 2 * HD)
    return pl.pallas_call(
        front_kernel,
        out_shape=(
            shape((REPLICAS, SLOT, HD), BF16),
            shape(other, BF16),
            shape((HELD,), I32),
        ),
        in_specs=[HBM] * 6,
        out_specs=(HBM, HBM, HBM),
        scratch_shapes=[
            pltpu.SMEM(dest.shape, I32),
            pltpu.SMEM(slots.shape, I32),
            pltpu.SMEM((HELD,), I32),
            pltpu.VMEM((2, HELD, KVH), BF16),
            pltpu.VMEM((HELD, 2, SPAN, KVH * HD), BF16),
            pltpu.VMEM((MOVE, SLOT, HD), BF16),
            pltpu.VMEM(other, BF16),
            pltpu.VMEM((2 * HELD, HD), F32),
            pltpu.SemaphoreType.DMA((4,)),
            pltpu.SemaphoreType.DMA((HELD, 2)),
            pltpu.SemaphoreType.DMA((MOVE,)),
            pltpu.SemaphoreType.DMA((2,)),
        ],
        cost_estimate=cost(1 << 20, 4 << 20),
        compiler_params=room(FRONT_ROOM),
        name="front",
    )(dest, slots, keys, values, key_scales, value_scales)


def unpack_kernel(
    plan, received, keys, values, key_scales, value_scales,
    new_keys, new_values, new_key_scales, new_value_scales,
    stage, scr, thin, in_sem, out_sem, thin_sem,
):
    def copies(r, inward):
        pairs = ((keys, new_keys), (values, new_values))
        if inward:
            return [
                pltpu.make_async_copy(old.at[r], stage.at[r, i], in_sem.at[r, i])
                for i, (old, _) in enumerate(pairs)
            ]
        return [
            pltpu.make_async_copy(stage.at[r, i], new.at[r], out_sem.at[r, i])
            for i, (_, new) in enumerate(pairs)
        ]

    for r in range(HELD):

        @pl.when(plan[r] < 0)
        def _():
            for copy in copies(r, True):
                copy.start()

    scale_rows(scr, key_scales, value_scales)
    for r in range(HELD):
        source = plan[r]

        @pl.when(source >= 0)
        def _():
            both = received[source, 2 * KVH * SPAN : SLOT, :].astype(F32)
            scr[r : r + 1, :] = both[0:1, :]
            scr[HELD + r : HELD + r + 1, :] = both[1:2, :]
            for which in range(2):
                for c in range(KVH):
                    at_row = (which * KVH + c) * SPAN
                    stage[r, which, :, c * HD : (c + 1) * HD] = received[
                        source, at_row : at_row + SPAN, :
                    ]
            for copy in copies(r, False):
                copy.start()

    thin[0] = scr[0:HELD, 0:KVH].astype(BF16)
    thin[1] = scr[HELD : 2 * HELD, 0:KVH].astype(BF16)
    scales_out = [
        pltpu.make_async_copy(thin.at[i], new, thin_sem.at[i])
        for i, new in enumerate((new_key_scales, new_value_scales))
    ]
    for copy in scales_out:
        copy.start()
    for r in range(HELD):

        @pl.when(plan[r] < 0)
        def _():
            for copy in copies(r, True):
                copy.wait()
            for copy in copies(r, False):
                copy.start()

    for r in range(HELD):
        for copy in copies(r, False):
            copy.wait()
    for copy in scales_out:
        copy.wait()


def unpack(plan, received, keys, values, key_scales, value_scales):
    return pl.pallas_call(
        unpack_kernel,
        out_shape=(
            shape(keys.shape, BF16),
            shape(values.shape, BF16),
            shape((HELD, KVH), BF16),
            shape((HELD, KVH), BF16),
        ),
        in_specs=[SMEM, VMEM, HBM, HBM, VMEM, VMEM],
        out_specs=(HBM, HBM, HBM, HBM),
        scratch_shapes=[
            pltpu.VMEM((HELD, 2, SPAN, KVH * HD), BF16),
            pltpu.VMEM((2 * HELD, HD), F32),
            pltpu.VMEM((2, HELD, KVH), BF16),
            pltpu.SemaphoreType.DMA((HELD, 2)),
            pltpu.SemaphoreType.DMA((HELD, 2)),
            pltpu.SemaphoreType.DMA((2,)),
        ],
        cost_estimate=cost(1 << 20, 4 << 20),
        compiler_params=room(8),
        name="unpack",
    )(plan, received, keys, values, key_scales, value_scales)


def query_kernel(hidden, weight, gain, query, residual, rows, blocks, rows_sem, block_sem):
    rank = lax.axis_index("tensor")
    depth = blocks.shape[1]
    rows_in = pltpu.make_async_copy(hidden, rows, rows_sem)
    rows_in.start()
    weights_in = []
    for i in range(STEPS):
        copy = pltpu.make_async_copy(
            weight.at[i * depth : (i + 1) * depth, :], blocks.at[i], block_sem.at[i]
        )
        copy.start()
        weights_in.append(copy)
    rows_in.wait()
    residual[...] = rows[:, pl.ds(pl.multiple_of(rank * COLS, COLS), COLS)]
    total = jnp.zeros((ROWS, 2 * HD), F32)
    for i in range(STEPS):
        weights_in[i].wait()
        total = total + jnp.dot(
            rows[:, i * depth : (i + 1) * depth], blocks[i], preferred_element_type=F32
        )
    for h in range(2):
        part = total[:, h * HD : (h + 1) * HD]
        mean = jnp.mean(part * part, axis=-1, keepdims=True)
        part = part * lax.rsqrt(mean + EPSILON)
        query[:, h * HD : (h + 1) * HD] = (part * gain[...] * HD ** (-0.5)).astype(BF16)


def project_query(hidden, q_weight, q_gain):
    depth = hidden.shape[1] // STEPS
    return pl.pallas_call(
        query_kernel,
        out_shape=(shape((ROWS, 2 * HD), BF16), shape((ROWS, COLS), BF16)),
        in_specs=[HBM, HBM, VMEM],
        out_specs=(VMEM, VMEM),
        scratch_shapes=[
            pltpu.VMEM(hidden.shape, BF16),
            pltpu.VMEM((STEPS, depth, 2 * HD), BF16),
            pltpu.SemaphoreType.DMA,
            pltpu.SemaphoreType.DMA((STEPS,)),
        ],
        cost_estimate=cost(1 << 22, 5 << 20),
        compiler_params=room(QUERY_ROOM),
        name="query",
    )(hidden, q_weight, q_gain.reshape(1, HD))


def split3(x):
    high = x.astype(BF16).astype(F32)
    rest = x - high
    middle = rest.astype(BF16).astype(F32)
    return high, middle, rest - middle


def put_stats(out, at_row, stats):
    high, middle, low = split3(stats)
    out[at_row : at_row + 16, :] = jnp.concatenate([high, middle], axis=0).astype(BF16)
    out[at_row + 16 : at_row + 32, :] = jnp.concatenate(
        [low, jnp.zeros_like(low)], axis=0
    ).astype(BF16)


def get_stats(message, at_row):
    first = message[at_row : at_row + 16, :].astype(F32)
    second = message[at_row + 16 : at_row + 32, :].astype(F32)
    return (first[0:8] + first[8:16]) + second[0:8]


def columns_of(rows):
    short = HD - rows.shape[0]
    return jnp.concatenate([rows, jnp.zeros((short, HD), F32)], axis=0).T


def attend_kernel(
    lengths, q0, q1, q2, q3, keys, values, key_scales, value_scales, other,
    o0, o1, o2, o3, q_all, o_all, mask, stats,
):
    rank = lax.axis_index("tensor")
    y = rank // 4
    x = (rank // 2) % 2
    for k, q in enumerate((q0, q1, q2, q3)):
        q_all[k] = q[...]
    tokens = HELD * SPAN
    row_request = (iota((HD, tokens), 0) // SPEC) % HELD
    col = iota((HD, tokens), 1)
    limit = jnp.zeros((1, tokens), I32)
    col1 = iota((1, tokens), 1)
    for r in range(HELD):
        limit = jnp.where(col1 // SPAN == r, lengths[r], limit)
    own_request = row_request == col // SPAN
    beside = rank + 2 - 4 * x
    for b, block in enumerate((rank, beside)):
        in_reach = block * SPAN + col1 % SPAN < limit
        mask[b] = jnp.where(jnp.logical_and(own_request, in_reach), 1.0, 0.0)
    spread_cols = (iota((HELD, tokens), 1) // SPAN == iota((HELD, tokens), 0)).astype(BF16)
    spread_rows = ((iota((HD, HELD), 0) // SPEC) % HELD == iota((HD, HELD), 1)).astype(BF16)
    end = 2 * tokens
    scales = (
        (key_scales[...], value_scales[...]),
        (other[end : end + HELD, 0:KVH], other[end + HELD : end + 2 * HELD, 0:KVH]),
    )
    col_scale = [
        lax.dot_general(
            k, spread_cols, (((0,), (0,)), ((), ())), preferred_element_type=F32
        )
        for k, _ in scales
    ]
    row_scale = [jnp.dot(spread_rows, v, preferred_element_type=F32) for _, v in scales]
    lane = iota((HD, HD), 1)
    stats[...] = jnp.zeros_like(stats)
    for i in range(KVH // 2):
        k = (y - i + 4) % 4
        near, far = q_all[k, 0], q_all[k, 1]
        grouped = jnp.concatenate(
            [near[:, :HD], near[:, HD:], far[:, :HD], far[:, HD:]], axis=0
        )
        start = pl.multiple_of((2 * i + x) * HD, HD)
        lanes = slice(i * HD, (i + 1) * HD)
        key = (keys[:, :, pl.ds(start, HD)].reshape(tokens, HD), other[0:tokens, lanes])
        value = (
            values[:, :, pl.ds(start, HD)].reshape(tokens, HD),
            other[tokens : 2 * tokens, lanes],
        )
        scores, peaks = [], []
        for b in range(2):
            across = jnp.where(
                x == 0, col_scale[b][2 * i : 2 * i + 1], col_scale[b][2 * i + 1 : 2 * i + 2]
            )
            score = across * lax.dot_general(
                grouped, key[b], (((1,), (1,)), ((), ())), preferred_element_type=F32
            )
            scores.append(score)
            masked = jnp.where(mask[b] > 0.5, score, NEGATIVE)
            peaks.append(jnp.max(masked, axis=1, keepdims=True))
        peak = jnp.maximum(*peaks)
        total, out = 0.0, 0.0
        for b in range(2):
            weight = jnp.where(mask[b] > 0.5, jnp.exp(scores[b] - peak), 0.0)
            total = total + jnp.sum(weight, axis=1, keepdims=True)
            down = jnp.where(
                x == 0, row_scale[b][:, 2 * i : 2 * i + 1], row_scale[b][:, 2 * i + 1 : 2 * i + 2]
            )
            out = out + down * jnp.dot(
                weight.astype(BF16), value[b], preferred_element_type=F32
            )
        o_all[k] = out.astype(BF16)
        stats[...] = jnp.where(
            lane == 8 * k, peak, jnp.where(lane == 8 * k + 1, total, stats[...])
        )
    turned = stats[...].T
    for k, o in enumerate((o0, o1, o2, o3)):
        o[0:HD, :] = o_all[k]
        put_stats(o, HD, turned[8 * k : 8 * k + 8])


def attend(lengths, queries, keys, values, key_scales, value_scales, other):
    out = shape((HD + 32, HD), BF16)
    return pl.pallas_call(
        attend_kernel,
        out_shape=(out,) * 4,
        in_specs=[SMEM] + [VMEM] * 9,
        out_specs=(VMEM,) * 4,
        scratch_shapes=[
            pltpu.VMEM((4, 2, ROWS, 2 * HD), BF16),
            pltpu.VMEM((4, HD, HD), BF16),
            pltpu.VMEM((2, HD, HELD * SPAN), F32),
            pltpu.VMEM((HD, HD), F32),
        ],
        cost_estimate=cost(4 << 20, 2 << 20),
        compiler_params=room(8),
        name="attend",
    )(lengths, *queries, keys, values, key_scales, value_scales, other)


def merged(stats):
    top = functools.reduce(jnp.maximum, stats)
    factors = [jnp.exp(s - top) for s in stats]
    total = sum(s * pltpu.roll(f, 1, 0) for s, f in zip(stats, factors))
    peak_row = iota(top.shape, 0) % 2 == 0
    return factors, jnp.where(peak_row, top, total)


def combine_kernel(p0, p1, p2, p3, o0, o1):
    parts = (p0, p1, p2, p3)
    factors, both = merged([get_stats(p, HD) for p in parts])
    column = columns_of(jnp.concatenate(factors, axis=0))
    summed = jnp.zeros((HD, HD), F32)
    for k, p in enumerate(parts):
        summed = summed + p[0:HD, :].astype(F32) * column[:, 8 * k : 8 * k + 1]
    for dc, o in enumerate((o0, o1)):
        o[0 : HD // 2, :] = summed[dc * 64 : dc * 64 + 64].astype(BF16)
        put_stats(o, HD // 2, both)


def combine(parts):
    out = shape((HD // 2 + 32, HD), BF16)
    return pl.pallas_call(
        combine_kernel,
        out_shape=(out,) * 2,
        in_specs=[VMEM] * 4,
        out_specs=(VMEM,) * 2,
        cost_estimate=cost(1 << 20, 1 << 19),
        compiler_params=room(4),
        name="combine",
    )(*parts)


def finished(parts):
    stats = []
    for d, p in enumerate(parts):
        s = get_stats(p, HD // 2)
        stats.append(pltpu.roll(s, HD // 2, 1) if d else s)
    factors, both = merged(stats)
    over = pltpu.roll(both, 7, 0)
    column = columns_of(jnp.concatenate([f / over for f in factors], axis=0))
    summed = jnp.zeros((HD // 2, HD), F32)
    for d, p in enumerate(parts):
        summed = summed + p[0 : HD // 2, :].astype(F32) * column[0 : HD // 2, 8 * d : 8 * d + 1]
    return summed.astype(BF16)


def half_in(core, weight, blocks, sem):
    copies = []
    for i in range(TENSORS // 2):
        start = pl.multiple_of((2 * i + core) * COLS, COLS)
        copy = pltpu.make_async_copy(weight.at[:, pl.ds(start, COLS)], blocks.at[i], sem.at[i])
        copy.start()
        copies.append(copy)
    return copies


def half_out(copies, attended, blocks, out):
    for i, copy in enumerate(copies):
        copy.wait()
        out[i] = jnp.dot(attended, blocks[i], preferred_element_type=F32).astype(out.dtype)


def output_other_kernel(p0, p1, weight, attended, out, blocks, sem):
    copies = half_in(1 - lax.axis_index("tensor") % 2, weight, blocks, sem)
    both = finished((p0, p1))
    for h in range(2):
        attended[:, h * HD : (h + 1) * HD] = both[h * ROWS : (h + 1) * ROWS]
    half_out(copies, attended[...], blocks, out)


def output_own_kernel(attended, weight, out, blocks, sem):
    copies = half_in(lax.axis_index("tensor") % 2, weight, blocks, sem)
    half_out(copies, attended[...], blocks, out)


HALF_SCRATCH = [
    pltpu.VMEM((TENSORS // 2, 2 * HD, COLS), BF16),
    pltpu.SemaphoreType.DMA((TENSORS // 2,)),
]


def output_other(parts, o_weight):
    return pl.pallas_call(
        output_other_kernel,
        out_shape=(
            shape((ROWS, 2 * HD), BF16),
            shape((TENSORS // 2, ROWS, COLS), BF16),
        ),
        in_specs=[VMEM] * 2 + [ANY],
        out_specs=(VMEM, VMEM),
        scratch_shapes=HALF_SCRATCH,
        cost_estimate=cost(1 << 22, 2 << 20),
        compiler_params=room(OUTPUT_ROOM),
        name="output_other",
    )(*parts, o_weight)


def output_own(attended, o_weight):
    return pl.pallas_call(
        output_own_kernel,
        out_shape=shape((TENSORS // 2, ROWS, COLS), F32),
        in_specs=[VMEM, ANY],
        out_specs=VMEM,
        scratch_shapes=HALF_SCRATCH,
        cost_estimate=cost(1 << 22, 2 << 20),
        compiler_params=room(OUTPUT_ROOM),
        name="output_own",
    )(attended, o_weight)


def share_kernel(own, received, keep, s1, s2, s3):
    y = lax.axis_index("tensor") // 4
    for k in range(4):
        group = (y - k + 4) % 4
        for c in range(2):
            value = own[2 * group + c] + received[2 * group + c].astype(F32)
            if k == 0:
                keep[c] = value
            else:
                (s1, s2, s3)[k - 1][c] = value.astype(BF16)


def share(own, received):
    out = shape((2, ROWS, COLS), BF16)
    return pl.pallas_call(
        share_kernel,
        out_shape=(shape((2, ROWS, COLS), F32), out, out, out),
        in_specs=[VMEM, VMEM],
        out_specs=(VMEM,) * 4,
        cost_estimate=cost(1 << 20, 1 << 20),
        compiler_params=room(6),
        name="share",
    )(own, received)


def narrow_kernel(own, r1, r2, r3, keep, send):
    x = (lax.axis_index("tensor") // 2) % 2
    for c, out in ((x, keep), (1 - x, send)):
        value = own[c] + r1[c].astype(F32) + r2[c].astype(F32) + r3[c].astype(F32)
        out[...] = value.astype(out.dtype)


def narrow(own, received):
    return pl.pallas_call(
        narrow_kernel,
        out_shape=(shape((ROWS, COLS), F32), shape((ROWS, COLS), BF16)),
        in_specs=[VMEM] * 4,
        out_specs=(VMEM,) * 2,
        cost_estimate=cost(1 << 20, 1 << 19),
        compiler_params=room(4),
        name="narrow",
    )(own, *received)


def mix_kernel(gate, own, received, residual, out):
    scale = jnp.tanh(jnp.full((8, HD), gate[0], F32))[0:1, 0:1]
    summed = own[...] + received[...].astype(F32)
    out[...] = (residual[...].astype(F32) + scale * summed).astype(BF16)


def mix(gate, own, received, residual):
    return pl.pallas_call(
        mix_kernel,
        out_shape=shape((ROWS, COLS), BF16),
        in_specs=[SMEM, VMEM, VMEM, VMEM],
        out_specs=VMEM,
        cost_estimate=cost(1 << 20, 1 << 18),
        compiler_params=room(4),
        name="mix",
    )(gate, own, received, residual)


def swap(array, bits):
    return lax.ppermute(array, "tensor", [(i, i ^ bits) for i in range(TENSORS)])


def shift(array, rows):
    return lax.ppermute(array, "tensor", [(i, (i + 4 * rows) % TENSORS) for i in range(TENSORS)])


def attention(
    hidden, q_weight, q_gain, o_weight, attn_gate,
    keys, values, key_scales, value_scales, other, lengths,
):
    query, residual = project_query(hidden, q_weight, q_gain)
    local = jnp.stack([query, swap(query, 1)])
    queries = [local] + [shift(local, k) for k in (1, 2, 3)]
    parts = attend(lengths, queries, keys, values, key_scales, value_scales, other)
    parts = combine([parts[0]] + [shift(parts[k], -k) for k in (1, 2, 3)])
    attended, sent = output_other([parts[0], swap(parts[1], 1)], o_weight)
    sent = swap(sent, 1)
    own, *sent = share(output_own(attended, o_weight), sent)
    own, sent = narrow(own, [shift(s, -k) for k, s in zip((1, 2, 3), sent)])
    return mix(attn_gate, own, swap(sent, 2), residual)


def local(
    hidden,
    q_weight,
    q_gain,
    o_weight,
    attn_gate,
    key_codes,
    value_codes,
    key_scales,
    value_scales,
    lengths,
    dest_replica,
    move_slot,
):
    dest = dest_replica.T
    key_scales, value_scales = key_scales[:, 0, :], value_scales[:, 0, :]
    message, other, plan = front(
        dest, move_slot, key_codes, value_codes, key_scales, value_scales
    )
    other = swap(other, 2)
    received = lax.all_to_all(
        message, "replica", split_axis=0, concat_axis=0, tiled=True
    )
    mixed = attention(
        hidden, q_weight, q_gain, o_weight, attn_gate,
        key_codes, value_codes, key_scales, value_scales, other, lengths,
    )
    new_keys, new_values, new_ks, new_vs = unpack(
        plan, received, key_codes, value_codes, key_scales, value_scales
    )
    return (mixed, new_keys, new_values, new_ks[:, None, :], new_vs[:, None, :])


def solution(mesh):
    return jax.shard_map(
        local,
        mesh=mesh,
        in_specs=(
            P("replica", None),
            P(None, "tensor"),
            P(),
            P("tensor", None),
            P(),
            P("replica", "tensor", None),
            P("replica", "tensor", None),
            P("replica", "tensor", None),
            P("replica", "tensor", None),
            P("replica"),
            P(),
            P("replica", None),
        ),
        out_specs=(
            P("replica", "tensor"),
            P("replica", "tensor", None),
            P("replica", "tensor", None),
            P("replica", "tensor", None),
            P("replica", "tensor", None),
        ),
        check_vma=False,
    )
```

```python
import functools

import jax
import jax.numpy as jnp
from jax import lax
from jax.experimental import pallas as pl
from jax.experimental.pallas import tpu as pltpu
from jax.sharding import PartitionSpec as P

NEGATIVE = -1e30
EPSILON = 1e-06
BF16, F32, I32 = jnp.bfloat16, jnp.float32, jnp.int32

REPLICAS = 16
MOVE = 6
HELD = 8
SPAN = 32
SPEC = 4
ROWS = HELD * SPEC
KVH = 8
HD = 128
TENSORS = 16
SLOT = 2 * KVH * SPAN + 8
COLS = 512
STEPS = 8
FRONT_ROOM, QUERY_ROOM, OUTPUT_ROOM = 57, 53.6, 51


VMEM = pl.BlockSpec(memory_space=pltpu.VMEM)
SMEM = pl.BlockSpec(memory_space=pltpu.SMEM)
HBM = pl.BlockSpec(memory_space=pltpu.HBM)
ANY = pl.BlockSpec(memory_space=pl.ANY)


def cost(flops, moved):
    return pl.CostEstimate(flops=flops, bytes_accessed=moved, transcendentals=0)


def room(mib):
    return pltpu.CompilerParams(vmem_limit_bytes=int(mib * (1 << 20)))


def shape(dims, dtype):
    return jax.ShapeDtypeStruct(dims, dtype)


def iota(dims, axis):
    return lax.broadcasted_iota(I32, dims, axis)


def scale_rows(scr, key_scales, value_scales):
    scr[...] = jnp.zeros_like(scr)
    scr[0:HELD, 0:KVH] = key_scales[...].astype(F32)
    scr[HELD : 2 * HELD, 0:KVH] = value_scales[...].astype(F32)


def front_kernel(
    dest_in, slots_in, keys, values, key_scales_in, value_scales_in,
    message, other_out, plan_out,
    dest, slots, plan, scales, held, stage, other, scr,
    small_sem, in_sem, out_sem, end_sem,
):
    here = lax.axis_index("replica")
    x = (lax.axis_index("tensor") // 2) % 2
    small = [
        pltpu.make_async_copy(source, target, small_sem.at[i])
        for i, (source, target) in enumerate(
            (
                (slots_in, slots),
                (dest_in, dest),
                (key_scales_in, scales.at[0]),
                (value_scales_in, scales.at[1]),
            )
        )
    ]
    for copy in small:
        copy.start()

    def loads(r):
        return (
            pltpu.make_async_copy(keys.at[r], held.at[r, 0], in_sem.at[r, 0]),
            pltpu.make_async_copy(values.at[r], held.at[r, 1], in_sem.at[r, 1]),
        )

    for r in range(HELD):
        for copy in loads(r):
            copy.start()
    for copy in small:
        copy.wait()
    for r in range(HELD):
        plan[r] = -1
    for j in range(MOVE):
        source = jnp.int32(0)
        for p in range(REPLICAS):
            source = jnp.where(dest[j, p] == here, p, source)
        plan[slots[0, j]] = source
    plan_copy = pltpu.make_async_copy(plan, plan_out, end_sem.at[0])
    plan_copy.start()
    scale_rows(scr, scales.at[0], scales.at[1])
    row = iota((8, HD), 0)
    for r in range(HELD):
        for copy in loads(r):
            copy.wait()
    stores = []
    for j in range(MOVE):
        s = slots[0, j]
        both = jnp.where(
            row == 0,
            scr[pl.ds(s, 1), :],
            jnp.where(row == 1, scr[pl.ds(HELD + s, 1), :], 0.0),
        )
        stage[j, 2 * KVH * SPAN : SLOT, :] = both.astype(BF16)
        for which in range(2):
            for c in range(KVH):
                at_row = (which * KVH + c) * SPAN
                stage[j, at_row : at_row + SPAN, :] = held[s, which, :, c * HD : (c + 1) * HD]
        copy = pltpu.make_async_copy(stage.at[j], message.at[dest[j, here]], out_sem.at[j])
        copy.start()
        stores.append(copy)
    for i in range(KVH // 2):
        start = pl.multiple_of((2 * i + 1 - x) * HD, HD)
        for which in range(2):
            for r in range(HELD):
                at_row = (which * HELD + r) * SPAN
                other[at_row : at_row + SPAN, i * HD : (i + 1) * HD] = held[
                    r, which, :, pl.ds(start, HD)
                ]
    other[2 * HELD * SPAN :, 0:HD] = scr[...].astype(BF16)
    other[2 * HELD * SPAN :, HD:] = jnp.zeros((2 * HELD, 3 * HD), BF16)
    other_copy = pltpu.make_async_copy(other, other_out, end_sem.at[1])
    other_copy.start()
    for copy in stores:
        copy.wait()
    plan_copy.wait()
    other_copy.wait()


def front(dest, slots, keys, values, key_scales, value_scales):
    other = (2 * HELD * SPAN + 2 * HELD, KVH // 2 * HD)
    return pl.pallas_call(
        front_kernel,
        out_shape=(
            shape((REPLICAS, SLOT, HD), BF16),
            shape(other, BF16),
            shape((HELD,), I32),
        ),
        in_specs=[HBM] * 6,
        out_specs=(HBM, HBM, HBM),
        scratch_shapes=[
            pltpu.SMEM(dest.shape, I32),
            pltpu.SMEM(slots.shape, I32),
            pltpu.SMEM((HELD,), I32),
            pltpu.VMEM((2, HELD, KVH), BF16),
            pltpu.VMEM((HELD, 2, SPAN, KVH * HD), BF16),
            pltpu.VMEM((MOVE, SLOT, HD), BF16),
            pltpu.VMEM(other, BF16),
            pltpu.VMEM((2 * HELD, HD), F32),
            pltpu.SemaphoreType.DMA((4,)),
            pltpu.SemaphoreType.DMA((HELD, 2)),
            pltpu.SemaphoreType.DMA((MOVE,)),
            pltpu.SemaphoreType.DMA((2,)),
        ],
        cost_estimate=cost(1 << 20, 4 << 20),
        compiler_params=room(FRONT_ROOM),
        name="front",
    )(dest, slots, keys, values, key_scales, value_scales)


def unpack_kernel(
    plan, received, keys, values, key_scales, value_scales,
    new_keys, new_values, new_key_scales, new_value_scales,
    stage, scr, thin, out_sem, thin_sem,
):
    pairs = ((keys, new_keys), (values, new_values))

    def stores(r, kept):
        return [
            pltpu.make_async_copy(old.at[r] if kept else stage.at[r, i], new.at[r], out_sem.at[r, i])
            for i, (old, new) in enumerate(pairs)
        ]

    for r in range(HELD):

        @pl.when(plan[r] < 0)
        def _():
            for copy in stores(r, True):
                copy.start()

    for r in range(HELD):
        source = plan[r]

        @pl.when(source >= 0)
        def _():
            for which in range(2):
                for c in range(KVH):
                    at_row = (which * KVH + c) * SPAN
                    stage[r, which, :, c * HD : (c + 1) * HD] = received[
                        source, at_row : at_row + SPAN, :
                    ]
            for copy in stores(r, False):
                copy.start()

    scale_rows(scr, key_scales, value_scales)
    for r in range(HELD):
        source = plan[r]

        @pl.when(source >= 0)
        def _():
            both = received[source, 2 * KVH * SPAN : SLOT, :].astype(F32)
            scr[r : r + 1, :] = both[0:1, :]
            scr[HELD + r : HELD + r + 1, :] = both[1:2, :]

    thin[0] = scr[0:HELD, 0:KVH].astype(BF16)
    thin[1] = scr[HELD : 2 * HELD, 0:KVH].astype(BF16)
    scales_out = [
        pltpu.make_async_copy(thin.at[i], new, thin_sem.at[i])
        for i, new in enumerate((new_key_scales, new_value_scales))
    ]
    for copy in scales_out:
        copy.start()
    for r in range(HELD):
        for copy in stores(r, False):
            copy.wait()
    for copy in scales_out:
        copy.wait()


def unpack(plan, received, keys, values, key_scales, value_scales):
    return pl.pallas_call(
        unpack_kernel,
        out_shape=(
            shape(keys.shape, BF16),
            shape(values.shape, BF16),
            shape((HELD, KVH), BF16),
            shape((HELD, KVH), BF16),
        ),
        in_specs=[SMEM, VMEM, VMEM, VMEM, VMEM, VMEM],
        out_specs=(HBM, HBM, HBM, HBM),
        scratch_shapes=[
            pltpu.VMEM((HELD, 2, SPAN, KVH * HD), BF16),
            pltpu.VMEM((2 * HELD, HD), F32),
            pltpu.VMEM((2, HELD, KVH), BF16),
            pltpu.SemaphoreType.DMA((HELD, 2)),
            pltpu.SemaphoreType.DMA((2,)),
        ],
        cost_estimate=cost(1 << 20, 4 << 20),
        compiler_params=room(8),
        name="unpack",
    )(plan, received, keys, values, key_scales, value_scales)


def query_kernel(hidden, weight, gain, query, residual, rows, blocks, rows_sem, block_sem):
    rank = lax.axis_index("tensor")
    depth = blocks.shape[1]
    rows_in = pltpu.make_async_copy(hidden, rows, rows_sem)
    rows_in.start()
    weights_in = []
    for i in range(STEPS):
        copy = pltpu.make_async_copy(
            weight.at[i * depth : (i + 1) * depth, :], blocks.at[i], block_sem.at[i]
        )
        copy.start()
        weights_in.append(copy)
    rows_in.wait()
    residual[...] = rows[:, pl.ds(pl.multiple_of(rank * COLS, COLS), COLS)]
    total = jnp.zeros((ROWS, 2 * HD), F32)
    for i in range(STEPS):
        weights_in[i].wait()
        total = total + jnp.dot(
            rows[:, i * depth : (i + 1) * depth], blocks[i], preferred_element_type=F32
        )
    for h in range(2):
        part = total[:, h * HD : (h + 1) * HD]
        mean = jnp.mean(part * part, axis=-1, keepdims=True)
        part = part * lax.rsqrt(mean + EPSILON)
        query[:, h * HD : (h + 1) * HD] = (part * gain[...] * HD ** (-0.5)).astype(BF16)


def project_query(hidden, q_weight, q_gain):
    depth = hidden.shape[1] // STEPS
    return pl.pallas_call(
        query_kernel,
        out_shape=(shape((ROWS, 2 * HD), BF16), shape((ROWS, COLS), BF16)),
        in_specs=[HBM, HBM, VMEM],
        out_specs=(VMEM, VMEM),
        scratch_shapes=[
            pltpu.VMEM(hidden.shape, BF16),
            pltpu.VMEM((STEPS, depth, 2 * HD), BF16),
            pltpu.SemaphoreType.DMA,
            pltpu.SemaphoreType.DMA((STEPS,)),
        ],
        cost_estimate=cost(1 << 22, 5 << 20),
        compiler_params=room(QUERY_ROOM),
        name="query",
    )(hidden, q_weight, q_gain.reshape(1, HD))


def split3(x):
    high = x.astype(BF16).astype(F32)
    rest = x - high
    middle = rest.astype(BF16).astype(F32)
    return high, middle, rest - middle


def put_stats(out, at_row, stats):
    high, middle, low = split3(stats)
    out[at_row : at_row + 16, :] = jnp.concatenate([high, middle], axis=0).astype(BF16)
    out[at_row + 16 : at_row + 32, :] = jnp.concatenate(
        [low, jnp.zeros_like(low)], axis=0
    ).astype(BF16)


def get_stats(message, at_row):
    first = message[at_row : at_row + 16, :].astype(F32)
    second = message[at_row + 16 : at_row + 32, :].astype(F32)
    return (first[0:8] + first[8:16]) + second[0:8]


def columns_of(rows):
    short = HD - rows.shape[0]
    return jnp.concatenate([rows, jnp.zeros((short, HD), F32)], axis=0).T


def attend_kernel(
    lengths, q0, q1, q2, q3, keys, values, key_scales, value_scales, other,
    o0, o1, o2, o3, q_all, o_all, mask, stats,
):
    rank = lax.axis_index("tensor")
    y = rank // 4
    x = (rank // 2) % 2
    for k, q in enumerate((q0, q1, q2, q3)):
        q_all[k] = q[...]
    tokens = HELD * SPAN
    row_request = (iota((HD, tokens), 0) // SPEC) % HELD
    col = iota((HD, tokens), 1)
    limit = jnp.zeros((1, tokens), I32)
    col1 = iota((1, tokens), 1)
    for r in range(HELD):
        limit = jnp.where(col1 // SPAN == r, lengths[r], limit)
    own_request = row_request == col // SPAN
    beside = rank + 2 - 4 * x
    for b, block in enumerate((rank, beside)):
        in_reach = block * SPAN + col1 % SPAN < limit
        mask[b] = jnp.where(jnp.logical_and(own_request, in_reach), 1.0, 0.0)
    spread_cols = (iota((HELD, tokens), 1) // SPAN == iota((HELD, tokens), 0)).astype(BF16)
    spread_rows = ((iota((HD, HELD), 0) // SPEC) % HELD == iota((HD, HELD), 1)).astype(BF16)
    end = 2 * tokens
    scales = (
        (key_scales[...], value_scales[...]),
        (other[end : end + HELD, 0:KVH], other[end + HELD : end + 2 * HELD, 0:KVH]),
    )
    col_scale = [
        lax.dot_general(
            k, spread_cols, (((0,), (0,)), ((), ())), preferred_element_type=F32
        )
        for k, _ in scales
    ]
    row_scale = [jnp.dot(spread_rows, v, preferred_element_type=F32) for _, v in scales]
    lane = iota((HD, HD), 1)
    stats[...] = jnp.zeros_like(stats)
    for i in range(KVH // 2):
        k = (y - i + 4) % 4
        near, far = q_all[k, 0], q_all[k, 1]
        grouped = jnp.concatenate(
            [near[:, :HD], near[:, HD:], far[:, :HD], far[:, HD:]], axis=0
        )
        start = pl.multiple_of((2 * i + x) * HD, HD)
        lanes = slice(i * HD, (i + 1) * HD)
        key = (keys[:, :, pl.ds(start, HD)].reshape(tokens, HD), other[0:tokens, lanes])
        value = (
            values[:, :, pl.ds(start, HD)].reshape(tokens, HD),
            other[tokens : 2 * tokens, lanes],
        )
        scores, peaks = [], []
        for b in range(2):
            across = jnp.where(
                x == 0, col_scale[b][2 * i : 2 * i + 1], col_scale[b][2 * i + 1 : 2 * i + 2]
            )
            score = across * lax.dot_general(
                grouped, key[b], (((1,), (1,)), ((), ())), preferred_element_type=F32
            )
            scores.append(score)
            masked = jnp.where(mask[b] > 0.5, score, NEGATIVE)
            peaks.append(jnp.max(masked, axis=1, keepdims=True))
        peak = jnp.maximum(*peaks)
        total, out = 0.0, 0.0
        for b in range(2):
            weight = jnp.where(mask[b] > 0.5, jnp.exp(scores[b] - peak), 0.0)
            total = total + jnp.sum(weight, axis=1, keepdims=True)
            down = jnp.where(
                x == 0, row_scale[b][:, 2 * i : 2 * i + 1], row_scale[b][:, 2 * i + 1 : 2 * i + 2]
            )
            out = out + down * jnp.dot(
                weight.astype(BF16), value[b], preferred_element_type=F32
            )
        o_all[k] = out.astype(BF16)
        stats[...] = jnp.where(
            lane == 8 * k, peak, jnp.where(lane == 8 * k + 1, total, stats[...])
        )
    turned = stats[...].T
    for k, o in enumerate((o0, o1, o2, o3)):
        o[0:HD, :] = o_all[k]
        put_stats(o, HD, turned[8 * k : 8 * k + 8])


def attend(lengths, queries, keys, values, key_scales, value_scales, other):
    out = shape((HD + 32, HD), BF16)
    return pl.pallas_call(
        attend_kernel,
        out_shape=(out,) * 4,
        in_specs=[SMEM] + [VMEM] * 9,
        out_specs=(VMEM,) * 4,
        scratch_shapes=[
            pltpu.VMEM((4, 2, ROWS, 2 * HD), BF16),
            pltpu.VMEM((4, HD, HD), BF16),
            pltpu.VMEM((2, HD, HELD * SPAN), F32),
            pltpu.VMEM((HD, HD), F32),
        ],
        cost_estimate=cost(4 << 20, 2 << 20),
        compiler_params=room(8),
        name="attend",
    )(lengths, *queries, keys, values, key_scales, value_scales, other)


def merged(stats):
    top = functools.reduce(jnp.maximum, stats)
    factors = [jnp.exp(s - top) for s in stats]
    total = sum(s * pltpu.roll(f, 1, 0) for s, f in zip(stats, factors))
    peak_row = iota(top.shape, 0) % 2 == 0
    return factors, jnp.where(peak_row, top, total)


def combine_kernel(p0, p1, p2, p3, o0, o1):
    parts = (p0, p1, p2, p3)
    factors, both = merged([get_stats(p, HD) for p in parts])
    column = columns_of(jnp.concatenate(factors, axis=0))
    summed = jnp.zeros((HD, HD), F32)
    for k, p in enumerate(parts):
        summed = summed + p[0:HD, :].astype(F32) * column[:, 8 * k : 8 * k + 1]
    for dc, o in enumerate((o0, o1)):
        o[0 : HD // 2, :] = summed[dc * 64 : dc * 64 + 64].astype(BF16)
        put_stats(o, HD // 2, both)


def combine(parts):
    out = shape((HD // 2 + 32, HD), BF16)
    return pl.pallas_call(
        combine_kernel,
        out_shape=(out,) * 2,
        in_specs=[VMEM] * 4,
        out_specs=(VMEM,) * 2,
        cost_estimate=cost(1 << 20, 1 << 19),
        compiler_params=room(4),
        name="combine",
    )(*parts)


def finished(parts):
    stats = []
    for d, p in enumerate(parts):
        s = get_stats(p, HD // 2)
        stats.append(pltpu.roll(s, HD // 2, 1) if d else s)
    factors, both = merged(stats)
    over = pltpu.roll(both, 7, 0)
    column = columns_of(jnp.concatenate([f / over for f in factors], axis=0))
    summed = jnp.zeros((HD // 2, HD), F32)
    for d, p in enumerate(parts):
        summed = summed + p[0 : HD // 2, :].astype(F32) * column[0 : HD // 2, 8 * d : 8 * d + 1]
    return summed.astype(BF16)


def half_in(core, weight, blocks, sem):
    copies = []
    for i in range(TENSORS // 2):
        start = pl.multiple_of((2 * i + core) * COLS, COLS)
        copy = pltpu.make_async_copy(weight.at[:, pl.ds(start, COLS)], blocks.at[i], sem.at[i])
        copy.start()
        copies.append(copy)
    return copies


def half_out(copies, attended, blocks, out):
    for i, copy in enumerate(copies):
        copy.wait()
        out[i] = jnp.dot(attended, blocks[i], preferred_element_type=F32).astype(out.dtype)


def output_other_kernel(p0, p1, weight, attended, out, blocks, sem):
    copies = half_in(1 - lax.axis_index("tensor") % 2, weight, blocks, sem)
    both = finished((p0, p1))
    for h in range(2):
        attended[:, h * HD : (h + 1) * HD] = both[h * ROWS : (h + 1) * ROWS]
    half_out(copies, attended[...], blocks, out)


def output_own_kernel(attended, weight, out, blocks, sem):
    copies = half_in(lax.axis_index("tensor") % 2, weight, blocks, sem)
    half_out(copies, attended[...], blocks, out)


HALF_SCRATCH = [
    pltpu.VMEM((TENSORS // 2, 2 * HD, COLS), BF16),
    pltpu.SemaphoreType.DMA((TENSORS // 2,)),
]


def output_other(parts, o_weight):
    return pl.pallas_call(
        output_other_kernel,
        out_shape=(
            shape((ROWS, 2 * HD), BF16),
            shape((TENSORS // 2, ROWS, COLS), BF16),
        ),
        in_specs=[VMEM] * 2 + [ANY],
        out_specs=(VMEM, VMEM),
        scratch_shapes=HALF_SCRATCH,
        cost_estimate=cost(1 << 22, 2 << 20),
        compiler_params=room(OUTPUT_ROOM),
        name="output_other",
    )(*parts, o_weight)


def output_own(attended, o_weight):
    return pl.pallas_call(
        output_own_kernel,
        out_shape=shape((TENSORS // 2, ROWS, COLS), F32),
        in_specs=[VMEM, ANY],
        out_specs=VMEM,
        scratch_shapes=HALF_SCRATCH,
        cost_estimate=cost(1 << 22, 2 << 20),
        compiler_params=room(OUTPUT_ROOM),
        name="output_own",
    )(attended, o_weight)


def share_kernel(own, received, keep, s1, s2, s3):
    y = lax.axis_index("tensor") // 4
    for k in range(4):
        group = (y - k + 4) % 4
        for c in range(2):
            value = own[2 * group + c] + received[2 * group + c].astype(F32)
            if k == 0:
                keep[c] = value
            else:
                (s1, s2, s3)[k - 1][c] = value.astype(BF16)


def share(own, received):
    out = shape((2, ROWS, COLS), BF16)
    return pl.pallas_call(
        share_kernel,
        out_shape=(shape((2, ROWS, COLS), F32), out, out, out),
        in_specs=[VMEM, VMEM],
        out_specs=(VMEM,) * 4,
        cost_estimate=cost(1 << 20, 1 << 20),
        compiler_params=room(6),
        name="share",
    )(own, received)


def narrow_kernel(own, r1, r2, r3, keep, send):
    x = (lax.axis_index("tensor") // 2) % 2
    for c, out in ((x, keep), (1 - x, send)):
        value = own[c] + r1[c].astype(F32) + r2[c].astype(F32) + r3[c].astype(F32)
        out[...] = value.astype(out.dtype)


def narrow(own, received):
    return pl.pallas_call(
        narrow_kernel,
        out_shape=(shape((ROWS, COLS), F32), shape((ROWS, COLS), BF16)),
        in_specs=[VMEM] * 4,
        out_specs=(VMEM,) * 2,
        cost_estimate=cost(1 << 20, 1 << 19),
        compiler_params=room(4),
        name="narrow",
    )(own, *received)


def mix_kernel(gate, own, received, residual, out):
    scale = jnp.tanh(jnp.full((8, HD), gate[0], F32))[0:1, 0:1]
    summed = own[...] + received[...].astype(F32)
    out[...] = (residual[...].astype(F32) + scale * summed).astype(BF16)


def mix(gate, own, received, residual):
    return pl.pallas_call(
        mix_kernel,
        out_shape=shape((ROWS, COLS), BF16),
        in_specs=[SMEM, VMEM, VMEM, VMEM],
        out_specs=VMEM,
        cost_estimate=cost(1 << 20, 1 << 18),
        compiler_params=room(4),
        name="mix",
    )(gate, own, received, residual)


def swap(array, bits):
    return lax.ppermute(array, "tensor", [(i, i ^ bits) for i in range(TENSORS)])


def shift(array, rows):
    return lax.ppermute(array, "tensor", [(i, (i + 4 * rows) % TENSORS) for i in range(TENSORS)])


def attention(
    hidden, q_weight, q_gain, o_weight, attn_gate,
    keys, values, key_scales, value_scales, other, lengths,
):
    query, residual = project_query(hidden, q_weight, q_gain)
    local = jnp.stack([query, swap(query, 1)])
    queries = [local] + [shift(local, k) for k in (1, 2, 3)]
    parts = attend(lengths, queries, keys, values, key_scales, value_scales, other)
    parts = combine([parts[0]] + [shift(parts[k], -k) for k in (1, 2, 3)])
    attended, sent = output_other([parts[0], swap(parts[1], 1)], o_weight)
    sent = swap(sent, 1)
    own, *sent = share(output_own(attended, o_weight), sent)
    own, sent = narrow(own, [shift(s, -k) for k, s in zip((1, 2, 3), sent)])
    return mix(attn_gate, own, swap(sent, 2), residual)


def local(
    hidden,
    q_weight,
    q_gain,
    o_weight,
    attn_gate,
    key_codes,
    value_codes,
    key_scales,
    value_scales,
    lengths,
    dest_replica,
    move_slot,
):
    dest = dest_replica.T
    key_scales, value_scales = key_scales[:, 0, :], value_scales[:, 0, :]
    message, other, plan = front(dest, move_slot, key_codes, value_codes, key_scales, value_scales)
    other = swap(other, 2)
    received = lax.all_to_all(
        message, "replica", split_axis=0, concat_axis=0, tiled=True
    )
    mixed = attention(
        hidden, q_weight, q_gain, o_weight, attn_gate,
        key_codes, value_codes, key_scales, value_scales, other, lengths,
    )
    new_keys, new_values, new_ks, new_vs = unpack(
        plan, received, key_codes, value_codes, key_scales, value_scales
    )
    return (mixed, new_keys, new_values, new_ks[:, None, :], new_vs[:, None, :])


def solution(mesh):
    return jax.shard_map(
        local,
        mesh=mesh,
        in_specs=(
            P("replica", None),
            P(None, "tensor"),
            P(),
            P("tensor", None),
            P(),
            P("replica", "tensor", None),
            P("replica", "tensor", None),
            P("replica", "tensor", None),
            P("replica", "tensor", None),
            P("replica"),
            P(),
            P("replica", None),
        ),
        out_specs=(
            P("replica", "tensor"),
            P("replica", "tensor", None),
            P("replica", "tensor", None),
            P("replica", "tensor", None),
            P("replica", "tensor", None),
        ),
        check_vma=False,
    )
```

```python
import functools

import jax
import jax.numpy as jnp
from jax import lax
from jax.experimental import pallas as pl
from jax.experimental.pallas import tpu as pltpu
from jax.sharding import PartitionSpec as P

NEGATIVE = -1e30
EPSILON = 1e-06
BF16, F32, I32 = jnp.bfloat16, jnp.float32, jnp.int32

REPLICAS = 16
MOVE = 6
HELD = 8
SPAN = 32
SPEC = 4
ROWS = HELD * SPEC
KVH = 8
HD = 128
TENSORS = 16
SLOT = 2 * KVH * SPAN + 8
COLS = 512
STEPS = 8
FRONT_ROOM, QUERY_ROOM, OUTPUT_ROOM = 57, 53.6, 51


VMEM = pl.BlockSpec(memory_space=pltpu.VMEM)
SMEM = pl.BlockSpec(memory_space=pltpu.SMEM)
HBM = pl.BlockSpec(memory_space=pltpu.HBM)
ANY = pl.BlockSpec(memory_space=pl.ANY)


def cost(flops, moved):
    return pl.CostEstimate(flops=flops, bytes_accessed=moved, transcendentals=0)


def room(mib):
    return pltpu.CompilerParams(vmem_limit_bytes=int(mib * (1 << 20)))


def shape(dims, dtype):
    return jax.ShapeDtypeStruct(dims, dtype)


def iota(dims, axis):
    return lax.broadcasted_iota(I32, dims, axis)


def scale_rows(scr, key_scales, value_scales):
    scr[...] = jnp.zeros_like(scr)
    scr[0:HELD, 0:KVH] = key_scales[...].astype(F32)
    scr[HELD : 2 * HELD, 0:KVH] = value_scales[...].astype(F32)


def front_kernel(
    dest_in, slots_in, keys, values, key_scales_in, value_scales_in,
    message, other_out, plan_out,
    dest, slots, plan, scales, held, stage, other, scr,
    small_sem, in_sem, out_sem, end_sem,
):
    here = lax.axis_index("replica")
    x = (lax.axis_index("tensor") // 2) % 2
    small = [
        pltpu.make_async_copy(source, target, small_sem.at[i])
        for i, (source, target) in enumerate(
            (
                (slots_in, slots),
                (dest_in, dest),
                (key_scales_in, scales.at[0]),
                (value_scales_in, scales.at[1]),
            )
        )
    ]
    for copy in small:
        copy.start()

    def loads(r):
        return (
            pltpu.make_async_copy(keys.at[r], held.at[r, 0], in_sem.at[r, 0]),
            pltpu.make_async_copy(values.at[r], held.at[r, 1], in_sem.at[r, 1]),
        )

    for r in range(HELD):
        for copy in loads(r):
            copy.start()
    for copy in small:
        copy.wait()
    for r in range(HELD):
        plan[r] = -1
    for j in range(MOVE):
        source = jnp.int32(0)
        for p in range(REPLICAS):
            source = jnp.where(dest[j, p] == here, p, source)
        plan[slots[0, j]] = source
    plan_copy = pltpu.make_async_copy(plan, plan_out, end_sem.at[0])
    plan_copy.start()
    scale_rows(scr, scales.at[0], scales.at[1])
    row = iota((8, HD), 0)
    stores = []
    for j in range(MOVE):
        s = slots[0, j]
        both = jnp.where(
            row == 0,
            scr[pl.ds(s, 1), :],
            jnp.where(row == 1, scr[pl.ds(HELD + s, 1), :], 0.0),
        )
        stage[j, 2 * KVH * SPAN : SLOT, :] = both.astype(BF16)
        for which, copy in enumerate(loads(s)):
            copy.wait()
            for c in range(KVH):
                at_row = (which * KVH + c) * SPAN
                stage[j, at_row : at_row + SPAN, :] = held[s, which, :, c * HD : (c + 1) * HD]
        copy = pltpu.make_async_copy(stage.at[j], message.at[dest[j, here]], out_sem.at[j])
        copy.start()
        stores.append(copy)
    for r in range(HELD):

        @pl.when(plan[r] < 0)
        def _():
            for copy in loads(r):
                copy.wait()

    for i in range(KVH // 2):
        start = pl.multiple_of((2 * i + 1 - x) * HD, HD)
        for which in range(2):
            for r in range(HELD):
                at_row = (which * HELD + r) * SPAN
                other[at_row : at_row + SPAN, i * HD : (i + 1) * HD] = held[
                    r, which, :, pl.ds(start, HD)
                ]
    other[2 * HELD * SPAN :, 0:HD] = scr[...].astype(BF16)
    other[2 * HELD * SPAN :, HD:] = jnp.zeros((2 * HELD, 3 * HD), BF16)
    other_copy = pltpu.make_async_copy(other, other_out, end_sem.at[1])
    other_copy.start()
    for copy in stores:
        copy.wait()
    plan_copy.wait()
    other_copy.wait()


def front(dest, slots, keys, values, key_scales, value_scales):
    other = (2 * HELD * SPAN + 2 * HELD, KVH // 2 * HD)
    return pl.pallas_call(
        front_kernel,
        out_shape=(
            shape((REPLICAS, SLOT, HD), BF16),
            shape(other, BF16),
            shape((HELD,), I32),
        ),
        in_specs=[HBM] * 6,
        out_specs=(HBM, HBM, HBM),
        scratch_shapes=[
            pltpu.SMEM(dest.shape, I32),
            pltpu.SMEM(slots.shape, I32),
            pltpu.SMEM((HELD,), I32),
            pltpu.VMEM((2, HELD, KVH), BF16),
            pltpu.VMEM((HELD, 2, SPAN, KVH * HD), BF16),
            pltpu.VMEM((MOVE, SLOT, HD), BF16),
            pltpu.VMEM(other, BF16),
            pltpu.VMEM((2 * HELD, HD), F32),
            pltpu.SemaphoreType.DMA((4,)),
            pltpu.SemaphoreType.DMA((HELD, 2)),
            pltpu.SemaphoreType.DMA((MOVE,)),
            pltpu.SemaphoreType.DMA((2,)),
        ],
        cost_estimate=cost(1 << 20, 4 << 20),
        compiler_params=room(FRONT_ROOM),
        name="front",
    )(dest, slots, keys, values, key_scales, value_scales)


def unpack_kernel(
    plan, received, keys, values, key_scales, value_scales,
    new_keys, new_values, new_key_scales, new_value_scales,
    stage, scr, thin, out_sem, thin_sem,
):
    pairs = ((keys, new_keys), (values, new_values))

    def stores(r, kept):
        return [
            pltpu.make_async_copy(old.at[r] if kept else stage.at[r, i], new.at[r], out_sem.at[r, i])
            for i, (old, new) in enumerate(pairs)
        ]

    for r in range(HELD):

        @pl.when(plan[r] < 0)
        def _():
            for copy in stores(r, True):
                copy.start()

    for r in range(HELD):
        source = plan[r]

        @pl.when(source >= 0)
        def _():
            for which in range(2):
                for c in range(KVH):
                    at_row = (which * KVH + c) * SPAN
                    stage[r, which, :, c * HD : (c + 1) * HD] = received[
                        source, at_row : at_row + SPAN, :
                    ]
            for copy in stores(r, False):
                copy.start()

    scale_rows(scr, key_scales, value_scales)
    for r in range(HELD):
        source = plan[r]

        @pl.when(source >= 0)
        def _():
            both = received[source, 2 * KVH * SPAN : SLOT, :].astype(F32)
            scr[r : r + 1, :] = both[0:1, :]
            scr[HELD + r : HELD + r + 1, :] = both[1:2, :]

    thin[0] = scr[0:HELD, 0:KVH].astype(BF16)
    thin[1] = scr[HELD : 2 * HELD, 0:KVH].astype(BF16)
    scales_out = [
        pltpu.make_async_copy(thin.at[i], new, thin_sem.at[i])
        for i, new in enumerate((new_key_scales, new_value_scales))
    ]
    for copy in scales_out:
        copy.start()
    for r in range(HELD):
        for copy in stores(r, False):
            copy.wait()
    for copy in scales_out:
        copy.wait()


def unpack(plan, received, keys, values, key_scales, value_scales):
    return pl.pallas_call(
        unpack_kernel,
        out_shape=(
            shape(keys.shape, BF16),
            shape(values.shape, BF16),
            shape((HELD, KVH), BF16),
            shape((HELD, KVH), BF16),
        ),
        in_specs=[SMEM, VMEM, VMEM, VMEM, VMEM, VMEM],
        out_specs=(HBM, HBM, HBM, HBM),
        scratch_shapes=[
            pltpu.VMEM((HELD, 2, SPAN, KVH * HD), BF16),
            pltpu.VMEM((2 * HELD, HD), F32),
            pltpu.VMEM((2, HELD, KVH), BF16),
            pltpu.SemaphoreType.DMA((HELD, 2)),
            pltpu.SemaphoreType.DMA((2,)),
        ],
        cost_estimate=cost(1 << 20, 4 << 20),
        compiler_params=room(8),
        name="unpack",
    )(plan, received, keys, values, key_scales, value_scales)


def query_kernel(hidden, weight, gain, query, residual, rows, blocks, rows_sem, block_sem):
    rank = lax.axis_index("tensor")
    depth = blocks.shape[1]
    rows_in = pltpu.make_async_copy(hidden, rows, rows_sem)
    rows_in.start()
    weights_in = []
    for i in range(STEPS):
        copy = pltpu.make_async_copy(
            weight.at[i * depth : (i + 1) * depth, :], blocks.at[i], block_sem.at[i]
        )
        copy.start()
        weights_in.append(copy)
    rows_in.wait()
    residual[...] = rows[:, pl.ds(pl.multiple_of(rank * COLS, COLS), COLS)]
    total = jnp.zeros((ROWS, 2 * HD), F32)
    for i in range(STEPS):
        weights_in[i].wait()
        total = total + jnp.dot(
            rows[:, i * depth : (i + 1) * depth], blocks[i], preferred_element_type=F32
        )
    for h in range(2):
        part = total[:, h * HD : (h + 1) * HD]
        mean = jnp.mean(part * part, axis=-1, keepdims=True)
        part = part * lax.rsqrt(mean + EPSILON)
        query[:, h * HD : (h + 1) * HD] = (part * gain[...] * HD ** (-0.5)).astype(BF16)


def project_query(hidden, q_weight, q_gain):
    depth = hidden.shape[1] // STEPS
    return pl.pallas_call(
        query_kernel,
        out_shape=(shape((ROWS, 2 * HD), BF16), shape((ROWS, COLS), BF16)),
        in_specs=[HBM, HBM, VMEM],
        out_specs=(VMEM, VMEM),
        scratch_shapes=[
            pltpu.VMEM(hidden.shape, BF16),
            pltpu.VMEM((STEPS, depth, 2 * HD), BF16),
            pltpu.SemaphoreType.DMA,
            pltpu.SemaphoreType.DMA((STEPS,)),
        ],
        cost_estimate=cost(1 << 22, 5 << 20),
        compiler_params=room(QUERY_ROOM),
        name="query",
    )(hidden, q_weight, q_gain.reshape(1, HD))


def split3(x):
    high = x.astype(BF16).astype(F32)
    rest = x - high
    middle = rest.astype(BF16).astype(F32)
    return high, middle, rest - middle


def put_stats(out, at_row, stats):
    high, middle, low = split3(stats)
    out[at_row : at_row + 16, :] = jnp.concatenate([high, middle], axis=0).astype(BF16)
    out[at_row + 16 : at_row + 32, :] = jnp.concatenate(
        [low, jnp.zeros_like(low)], axis=0
    ).astype(BF16)


def get_stats(message, at_row):
    first = message[at_row : at_row + 16, :].astype(F32)
    second = message[at_row + 16 : at_row + 32, :].astype(F32)
    return (first[0:8] + first[8:16]) + second[0:8]


def columns_of(rows):
    short = HD - rows.shape[0]
    return jnp.concatenate([rows, jnp.zeros((short, HD), F32)], axis=0).T


def attend_kernel(
    lengths, q0, q1, q2, q3, keys, values, key_scales, value_scales, other,
    o0, o1, o2, o3, q_all, o_all, mask, stats,
):
    rank = lax.axis_index("tensor")
    y = rank // 4
    x = (rank // 2) % 2
    for k, q in enumerate((q0, q1, q2, q3)):
        q_all[k] = q[...]
    tokens = HELD * SPAN
    row_request = (iota((HD, tokens), 0) // SPEC) % HELD
    col = iota((HD, tokens), 1)
    limit = jnp.zeros((1, tokens), I32)
    col1 = iota((1, tokens), 1)
    for r in range(HELD):
        limit = jnp.where(col1 // SPAN == r, lengths[r], limit)
    own_request = row_request == col // SPAN
    beside = rank + 2 - 4 * x
    for b, block in enumerate((rank, beside)):
        in_reach = block * SPAN + col1 % SPAN < limit
        mask[b] = jnp.where(jnp.logical_and(own_request, in_reach), 1.0, 0.0)
    spread_cols = (iota((HELD, tokens), 1) // SPAN == iota((HELD, tokens), 0)).astype(BF16)
    spread_rows = ((iota((HD, HELD), 0) // SPEC) % HELD == iota((HD, HELD), 1)).astype(BF16)
    end = 2 * tokens
    scales = (
        (key_scales[...], value_scales[...]),
        (other[end : end + HELD, 0:KVH], other[end + HELD : end + 2 * HELD, 0:KVH]),
    )
    col_scale = [
        lax.dot_general(
            k, spread_cols, (((0,), (0,)), ((), ())), preferred_element_type=F32
        )
        for k, _ in scales
    ]
    row_scale = [jnp.dot(spread_rows, v, preferred_element_type=F32) for _, v in scales]
    lane = iota((HD, HD), 1)
    stats[...] = jnp.zeros_like(stats)
    for i in range(KVH // 2):
        k = (y - i + 4) % 4
        near, far = q_all[k, 0], q_all[k, 1]
        grouped = jnp.concatenate(
            [near[:, :HD], near[:, HD:], far[:, :HD], far[:, HD:]], axis=0
        )
        start = pl.multiple_of((2 * i + x) * HD, HD)
        lanes = slice(i * HD, (i + 1) * HD)
        key = (keys[:, :, pl.ds(start, HD)].reshape(tokens, HD), other[0:tokens, lanes])
        value = (
            values[:, :, pl.ds(start, HD)].reshape(tokens, HD),
            other[tokens : 2 * tokens, lanes],
        )
        scores, peaks = [], []
        for b in range(2):
            across = jnp.where(
                x == 0, col_scale[b][2 * i : 2 * i + 1], col_scale[b][2 * i + 1 : 2 * i + 2]
            )
            score = across * lax.dot_general(
                grouped, key[b], (((1,), (1,)), ((), ())), preferred_element_type=F32
            )
            scores.append(score)
            masked = jnp.where(mask[b] > 0.5, score, NEGATIVE)
            peaks.append(jnp.max(masked, axis=1, keepdims=True))
        peak = jnp.maximum(*peaks)
        total, out = 0.0, 0.0
        for b in range(2):
            weight = jnp.where(mask[b] > 0.5, jnp.exp(scores[b] - peak), 0.0)
            total = total + jnp.sum(weight, axis=1, keepdims=True)
            down = jnp.where(
                x == 0, row_scale[b][:, 2 * i : 2 * i + 1], row_scale[b][:, 2 * i + 1 : 2 * i + 2]
            )
            out = out + down * jnp.dot(
                weight.astype(BF16), value[b], preferred_element_type=F32
            )
        o_all[k] = out.astype(BF16)
        stats[...] = jnp.where(
            lane == 8 * k, peak, jnp.where(lane == 8 * k + 1, total, stats[...])
        )
    turned = stats[...].T
    for k, o in enumerate((o0, o1, o2, o3)):
        o[0:HD, :] = o_all[k]
        put_stats(o, HD, turned[8 * k : 8 * k + 8])


def attend(lengths, queries, keys, values, key_scales, value_scales, other):
    out = shape((HD + 32, HD), BF16)
    return pl.pallas_call(
        attend_kernel,
        out_shape=(out,) * 4,
        in_specs=[SMEM] + [VMEM] * 9,
        out_specs=(VMEM,) * 4,
        scratch_shapes=[
            pltpu.VMEM((4, 2, ROWS, 2 * HD), BF16),
            pltpu.VMEM((4, HD, HD), BF16),
            pltpu.VMEM((2, HD, HELD * SPAN), F32),
            pltpu.VMEM((HD, HD), F32),
        ],
        cost_estimate=cost(4 << 20, 2 << 20),
        compiler_params=room(8),
        name="attend",
    )(lengths, *queries, keys, values, key_scales, value_scales, other)


def merged(stats):
    top = functools.reduce(jnp.maximum, stats)
    factors = [jnp.exp(s - top) for s in stats]
    total = sum(s * pltpu.roll(f, 1, 0) for s, f in zip(stats, factors))
    peak_row = iota(top.shape, 0) % 2 == 0
    return factors, jnp.where(peak_row, top, total)


def combine_kernel(p0, p1, p2, p3, o0, o1):
    parts = (p0, p1, p2, p3)
    factors, both = merged([get_stats(p, HD) for p in parts])
    column = columns_of(jnp.concatenate(factors, axis=0))
    summed = jnp.zeros((HD, HD), F32)
    for k, p in enumerate(parts):
        summed = summed + p[0:HD, :].astype(F32) * column[:, 8 * k : 8 * k + 1]
    for dc, o in enumerate((o0, o1)):
        o[0 : HD // 2, :] = summed[dc * 64 : dc * 64 + 64].astype(BF16)
        put_stats(o, HD // 2, both)


def combine(parts):
    out = shape((HD // 2 + 32, HD), BF16)
    return pl.pallas_call(
        combine_kernel,
        out_shape=(out,) * 2,
        in_specs=[VMEM] * 4,
        out_specs=(VMEM,) * 2,
        cost_estimate=cost(1 << 20, 1 << 19),
        compiler_params=room(4),
        name="combine",
    )(*parts)


def finished(parts):
    stats = []
    for d, p in enumerate(parts):
        s = get_stats(p, HD // 2)
        stats.append(pltpu.roll(s, HD // 2, 1) if d else s)
    factors, both = merged(stats)
    over = pltpu.roll(both, 7, 0)
    column = columns_of(jnp.concatenate([f / over for f in factors], axis=0))
    summed = jnp.zeros((HD // 2, HD), F32)
    for d, p in enumerate(parts):
        summed = summed + p[0 : HD // 2, :].astype(F32) * column[0 : HD // 2, 8 * d : 8 * d + 1]
    return summed.astype(BF16)


def half_in(core, weight, blocks, sem):
    copies = []
    for i in range(TENSORS // 2):
        start = pl.multiple_of((2 * i + core) * COLS, COLS)
        copy = pltpu.make_async_copy(weight.at[:, pl.ds(start, COLS)], blocks.at[i], sem.at[i])
        copy.start()
        copies.append(copy)
    return copies


def half_out(copies, attended, blocks, out):
    for i, copy in enumerate(copies):
        copy.wait()
        out[i] = jnp.dot(attended, blocks[i], preferred_element_type=F32).astype(out.dtype)


def output_other_kernel(p0, p1, weight, attended, out, blocks, sem):
    copies = half_in(1 - lax.axis_index("tensor") % 2, weight, blocks, sem)
    both = finished((p0, p1))
    for h in range(2):
        attended[:, h * HD : (h + 1) * HD] = both[h * ROWS : (h + 1) * ROWS]
    half_out(copies, attended[...], blocks, out)


def output_own_kernel(attended, weight, out, blocks, sem):
    copies = half_in(lax.axis_index("tensor") % 2, weight, blocks, sem)
    half_out(copies, attended[...], blocks, out)


HALF_SCRATCH = [
    pltpu.VMEM((TENSORS // 2, 2 * HD, COLS), BF16),
    pltpu.SemaphoreType.DMA((TENSORS // 2,)),
]


def output_other(parts, o_weight):
    return pl.pallas_call(
        output_other_kernel,
        out_shape=(
            shape((ROWS, 2 * HD), BF16),
            shape((TENSORS // 2, ROWS, COLS), BF16),
        ),
        in_specs=[VMEM] * 2 + [ANY],
        out_specs=(VMEM, VMEM),
        scratch_shapes=HALF_SCRATCH,
        cost_estimate=cost(1 << 22, 2 << 20),
        compiler_params=room(OUTPUT_ROOM),
        name="output_other",
    )(*parts, o_weight)


def output_own(attended, o_weight):
    return pl.pallas_call(
        output_own_kernel,
        out_shape=shape((TENSORS // 2, ROWS, COLS), F32),
        in_specs=[VMEM, ANY],
        out_specs=VMEM,
        scratch_shapes=HALF_SCRATCH,
        cost_estimate=cost(1 << 22, 2 << 20),
        compiler_params=room(OUTPUT_ROOM),
        name="output_own",
    )(attended, o_weight)


def share_kernel(own, received, keep, s1, s2, s3):
    y = lax.axis_index("tensor") // 4
    for k in range(4):
        group = (y - k + 4) % 4
        for c in range(2):
            value = own[2 * group + c] + received[2 * group + c].astype(F32)
            if k == 0:
                keep[c] = value
            else:
                (s1, s2, s3)[k - 1][c] = value.astype(BF16)


def share(own, received):
    out = shape((2, ROWS, COLS), BF16)
    return pl.pallas_call(
        share_kernel,
        out_shape=(shape((2, ROWS, COLS), F32), out, out, out),
        in_specs=[VMEM, VMEM],
        out_specs=(VMEM,) * 4,
        cost_estimate=cost(1 << 20, 1 << 20),
        compiler_params=room(6),
        name="share",
    )(own, received)


def narrow_kernel(own, r1, r2, r3, keep, send):
    x = (lax.axis_index("tensor") // 2) % 2
    for c, out in ((x, keep), (1 - x, send)):
        value = own[c] + r1[c].astype(F32) + r2[c].astype(F32) + r3[c].astype(F32)
        out[...] = value.astype(out.dtype)


def narrow(own, received):
    return pl.pallas_call(
        narrow_kernel,
        out_shape=(shape((ROWS, COLS), F32), shape((ROWS, COLS), BF16)),
        in_specs=[VMEM] * 4,
        out_specs=(VMEM,) * 2,
        cost_estimate=cost(1 << 20, 1 << 19),
        compiler_params=room(4),
        name="narrow",
    )(own, *received)


def mix_kernel(gate, own, received, residual, out):
    scale = jnp.tanh(jnp.full((8, HD), gate[0], F32))[0:1, 0:1]
    summed = own[...] + received[...].astype(F32)
    out[...] = (residual[...].astype(F32) + scale * summed).astype(BF16)


def mix(gate, own, received, residual):
    return pl.pallas_call(
        mix_kernel,
        out_shape=shape((ROWS, COLS), BF16),
        in_specs=[SMEM, VMEM, VMEM, VMEM],
        out_specs=VMEM,
        cost_estimate=cost(1 << 20, 1 << 18),
        compiler_params=room(4),
        name="mix",
    )(gate, own, received, residual)


def swap(array, bits):
    return lax.ppermute(array, "tensor", [(i, i ^ bits) for i in range(TENSORS)])


def shift(array, rows):
    return lax.ppermute(array, "tensor", [(i, (i + 4 * rows) % TENSORS) for i in range(TENSORS)])


def attention(
    hidden, q_weight, q_gain, o_weight, attn_gate,
    keys, values, key_scales, value_scales, other, lengths,
):
    query, residual = project_query(hidden, q_weight, q_gain)
    local = jnp.stack([query, swap(query, 1)])
    queries = [local] + [shift(local, k) for k in (1, 2, 3)]
    parts = attend(lengths, queries, keys, values, key_scales, value_scales, other)
    parts = combine([parts[0]] + [shift(parts[k], -k) for k in (1, 2, 3)])
    attended, sent = output_other([parts[0], swap(parts[1], 1)], o_weight)
    sent = swap(sent, 1)
    own, *sent = share(output_own(attended, o_weight), sent)
    own, sent = narrow(own, [shift(s, -k) for k, s in zip((1, 2, 3), sent)])
    return mix(attn_gate, own, swap(sent, 2), residual)


def local(
    hidden,
    q_weight,
    q_gain,
    o_weight,
    attn_gate,
    key_codes,
    value_codes,
    key_scales,
    value_scales,
    lengths,
    dest_replica,
    move_slot,
):
    dest = dest_replica.T
    key_scales, value_scales = key_scales[:, 0, :], value_scales[:, 0, :]
    message, other, plan = front(dest, move_slot, key_codes, value_codes, key_scales, value_scales)
    other = swap(other, 2)
    received = lax.all_to_all(
        message, "replica", split_axis=0, concat_axis=0, tiled=True
    )
    mixed = attention(
        hidden, q_weight, q_gain, o_weight, attn_gate,
        key_codes, value_codes, key_scales, value_scales, other, lengths,
    )
    new_keys, new_values, new_ks, new_vs = unpack(
        plan, received, key_codes, value_codes, key_scales, value_scales
    )
    return (mixed, new_keys, new_values, new_ks[:, None, :], new_vs[:, None, :])


def solution(mesh):
    return jax.shard_map(
        local,
        mesh=mesh,
        in_specs=(
            P("replica", None),
            P(None, "tensor"),
            P(),
            P("tensor", None),
            P(),
            P("replica", "tensor", None),
            P("replica", "tensor", None),
            P("replica", "tensor", None),
            P("replica", "tensor", None),
            P("replica"),
            P(),
            P("replica", None),
        ),
        out_specs=(
            P("replica", "tensor"),
            P("replica", "tensor", None),
            P("replica", "tensor", None),
            P("replica", "tensor", None),
            P("replica", "tensor", None),
        ),
        check_vma=False,
    )
```
